256 devices in a mesh: band: 8 (over y, core), fft: 32 (over x, z).
Axes of the slice: x: 4, y: 4, z: 8, core: 2. Of those that a mesh axis runs over, the one named last changes fastest.
Arguments:
- start_bands: float32 [2, 16, 96, 9216], P(None, 'band', 'fft'), may hold values from -6 to 6
- potential: float32 [96, 96, 96], P(None, None, 'fft'), may hold values from -2 to 1
- half_height: int32 [96, 96], P('fft'), may hold values from -1 to 24, as said below
- lower_bound: float32 [1], replicated, may hold values from 1 to 2
- upper_bound: float32 [1], replicated, may hold values from 14 to 16
- fermi_level: float32 [1], replicated, may hold values from 0 to 2
Outputs:
- filtered_bands: float32 [2, 16, 96, 9216], P(None, 'band', 'fft')
- energies: float32 [16], P('band')
- band_energy: float32 [1], replicated
The draws below stay inside these ranges and needn't reach their ends.
Inputs may be any that keep to these rules, and one draw needn't show every extreme that they name: Column (x, y) keeps exactly the wave vectors whose z frequency f has |f| <= half_height[x, y]; -1 marks an empty column; the column of x = y = 0 holds 24; every column whose x or y frequency exceeds 96/4 in magnitude is empty.
All inputs are finite; a program needn't handle non-finite values.
Results may differ from the reference program's by a relative error of at most 0.0003.
Values sent between devices are 32-bit elements; how exact they have to be, the bound alone decides.
A program may use at most 64 MiB of HBM per device.

```python
import jax
import jax.numpy as jnp
from jax import lax

NG = 96
DEGREE = 3
BANDS = 16
CELLS = 884736


def draw_half_height(key, part):
    quarter = NG // 4
    radius_sq = quarter * quarter + jax.random.randint(key, (), 0, quarter, dtype=jnp.int32)
    positions = jnp.arange(NG, dtype=jnp.int32)
    frequency = jnp.where(positions < NG // 2, positions, positions - NG)
    remaining = radius_sq - frequency[:, None] ** 2 - frequency[None, :] ** 2
    z_values = jnp.arange(NG // 2, dtype=jnp.int32)
    z_count = jnp.sum((z_values[None, None, :] ** 2 <= remaining[:, :, None]).astype(jnp.int32), axis=2)
    return z_count - 1


def shard_levels(key, extent, shards, smallest, largest):
    def one(position, parts):
        heights = jax.random.uniform(jax.random.fold_in(jax.random.fold_in(key, 6), position), (parts,), jnp.float32, smallest / len(shards), largest / len(shards))
        return jnp.repeat(jnp.exp(heights), extent[position] // parts).reshape((-1,) + (1,) * (len(extent) - position - 1))

    level = one(*shards[0])
    for cut in shards[1:]:
        level = level * one(*cut)
    return level


def scatter_about(key, extent, spread, most, split=(), held_as=jnp.bfloat16):
    gain = shard_levels(key, extent, split, -0.22, 0.18) if split else 1.0
    result = jax.random.normal(key, extent, jnp.float32) * spread * gain
    return jnp.minimum(jnp.maximum(result, -most), most).astype(held_as)


def setup_inputs(seed: int = 0) -> dict:
    key_list = jax.random.split(jax.random.key(seed), 7)
    return {
        "start_bands": scatter_about(key_list[0], (2, BANDS, NG, NG * NG), 1.0, 6.0, ((1, 8), (2, 32)), jnp.float32),
        "potential": jnp.clip(-2.0 + 3.0 * jax.random.uniform(key_list[1], (NG, NG, NG), jnp.float32) ** shard_levels(key_list[1], (NG, NG, NG), ((2, 32),), -0.2, 0.2), -2.0, 1.0),
        "half_height": draw_half_height(jax.random.fold_in(key_list[6], 71), 0),
        "lower_bound": jnp.clip(jax.random.uniform(key_list[3], (1,), jnp.float32, 1.0, 2.0), 1.0, 2.0),
        "upper_bound": jnp.clip(jax.random.uniform(key_list[4], (1,), jnp.float32, 14.0, 16.0), 14.0, 16.0),
        "fermi_level": jnp.clip(jax.random.uniform(key_list[5], (1,), jnp.float32, 0.0, 2.0), 0.0, 2.0),
    }


KIN_MAX = 12.0
TEMPER = 0.5
HIGHEST = lax.Precision.HIGHEST

def frequency_of(length):
    positions = jnp.arange(length, dtype=jnp.int32)
    return jnp.where(positions < length // 2, positions, positions - length)

def sphere_tables(half_height):
    frequency = frequency_of(NG)
    inside = (jnp.abs(frequency)[None, None, :] <= half_height[:, :, None]).astype(jnp.float32)
    squared = frequency[:, None, None] ** 2 + frequency[None, :, None] ** 2 + frequency[None, None, :] ** 2
    kinetic = KIN_MAX / (NG // 4) ** 2 * squared.astype(jnp.float32)
    return (inside, kinetic)

def hamiltonian(field, potential, inside, kinetic):

    def one_band(pair_parts):
        real_part, imag_part = pair_parts
        space = jnp.fft.ifftn(lax.complex(real_part, imag_part)) * potential
        back = jnp.fft.fftn(space)
        return (inside * (kinetic * real_part + jnp.real(back)), inside * (kinetic * imag_part + jnp.imag(back)))
    real_out, imag_out = lax.map(one_band, (field[0], field[1]))
    return jnp.stack([real_out, imag_out])

def reference(start_bands, potential, half_height, lower_bound, upper_bound, fermi_level):
    shaped = start_bands.reshape(2, BANDS, NG, NG, NG)
    inside, kinetic = sphere_tables(half_height)
    center = 0.5 * (upper_bound[0] + lower_bound[0])
    half_width = 0.5 * (upper_bound[0] - lower_bound[0])
    previous = inside * shaped
    current = (hamiltonian(previous, potential, inside, kinetic) - center * previous) / half_width
    for degree_step in range(1, DEGREE):
        following = 2.0 * (hamiltonian(current, potential, inside, kinetic) - center * current) / half_width - previous
        previous, current = (current, following)
    real_rows = current[0].reshape(BANDS, CELLS)
    imag_rows = current[1].reshape(BANDS, CELLS)
    gram_real = (jnp.dot(real_rows, real_rows.T, precision=HIGHEST) + jnp.dot(imag_rows, imag_rows.T, precision=HIGHEST)) / CELLS
    gram_imag = (jnp.dot(real_rows, imag_rows.T, precision=HIGHEST) - jnp.dot(imag_rows, real_rows.T, precision=HIGHEST)) / CELLS
    embedded = jnp.block([[gram_real, -gram_imag], [gram_imag, gram_real]])
    factor = jnp.linalg.cholesky(embedded)
    selector = jnp.eye(2 * BANDS, BANDS, dtype=jnp.float32)
    inverse_cols = lax.linalg.triangular_solve(factor, selector, left_side=True, lower=True, transpose_a=True)
    upper_rows = inverse_cols[:BANDS]
    lower_rows = inverse_cols[BANDS:]
    rot_real = jnp.dot(upper_rows.T, real_rows, precision=HIGHEST) - jnp.dot(lower_rows.T, imag_rows, precision=HIGHEST)
    rot_imag = jnp.dot(upper_rows.T, imag_rows, precision=HIGHEST) + jnp.dot(lower_rows.T, real_rows, precision=HIGHEST)
    rotated = jnp.stack([rot_real, rot_imag]).reshape(2, BANDS, NG, NG, NG)
    applied = hamiltonian(rotated, potential, inside, kinetic)
    energies = jnp.sum((rotated * applied).reshape(2, BANDS, CELLS), axis=(0, 2)) / CELLS
    weights = jax.nn.sigmoid((fermi_level[0] - energies) / TEMPER)
    band_energy = (jnp.sum(weights * energies) / BANDS).reshape(1)
    return (rotated.reshape(2, BANDS, NG, NG * NG), energies, band_energy)
```

```python
import math

import jax
import jax.numpy as jnp
import ml_dtypes
import numpy as np
from jax import lax
from jax.experimental import pallas as pl
from jax.experimental.pallas import tpu as pltpu
from jax.sharding import PartitionSpec as P

NG = 96
CELLS = float(NG**3)
BOX = 49
KIN = 12.0 / 24**2
TEMPER = 0.5
BANDS = 16
MEMBERS = 16
HOLDERS = 7
ZP = 6
F32, BF16 = jnp.float32, jnp.bfloat16
MESH = pl.DeviceIdType.MESH


def box_frequency():
    r = np.arange(BOX)
    return np.where(r <= 24, r, r - BOX)


def halves(table):
    table = table.astype(np.float32)
    high = table.astype(ml_dtypes.bfloat16)
    low = (table - high.astype(np.float32)).astype(ml_dtypes.bfloat16)
    return high, low


def tables():
    freq = box_frequency()
    angle = 2.0 * math.pi / NG * ((np.arange(NG)[:, None] * freq[None, :]) % NG)
    cosine, sine = np.cos(angle), np.sin(angle)
    ahead = np.zeros((192, 64))
    ahead[:96, :BOX], ahead[96:, :BOX] = cosine, sine
    back = np.zeros((128, 96))
    back[:BOX], back[64 : 64 + BOX] = cosine.T, sine.T
    lanes = np.zeros((128, 256))
    lanes[:BOX, :96], lanes[:BOX, 128:224] = cosine.T, sine.T
    lanes[64 : 64 + BOX, :96], lanes[64 : 64 + BOX, 128:224] = -sine.T, cosine.T
    lanes_back = lanes.T.copy()

    def left(t):
        high, low = halves(t)
        return np.concatenate([high, high, low], axis=1)

    def right(t):
        high, low = halves(t)
        return np.concatenate([high, high, low], axis=0)

    return left(ahead), left(back), right(lanes), right(lanes_back)


def split(x):
    high = x.astype(BF16)
    return high, (x - high.astype(F32)).astype(BF16)


def pieces(x, axis):
    high, low = split(x)
    return jnp.concatenate([high, low, high], axis=axis)


def dot(a, b):
    return jnp.dot(a, b, preferred_element_type=F32)


def dot_t(a, b):
    return lax.dot_general(a, b, (((1,), (1,)), ((), ())), preferred_element_type=F32)


def kernel(
    lower_ref,
    upper_ref,
    xi_ref,
    v_ref,
    ta_ref,
    tb_ref,
    ty_ref,
    tyb_ref,
    out_ref,
    energy_ref,
    xt,
    x0,
    vb,
    cur,
    prev,
    hy,
    inside,
    kin,
    sbuf,
    rbuf,
    bbuf,
    kbuf,
    gy,
    bh,
    bl,
    part,
    col,
    csum,
    full,
    qs,
    ob,
    s_init,
    r_init,
    s_v,
    r_v,
    s_f,
    r_f,
    s_b,
    r_b,
    s_g,
    r_g,
    s_c,
    r_c,
    s_p,
    r_p,
    s_o,
    r_o,
):
    p = lax.axis_index("band")
    i = lax.axis_index("fft")
    y, core = p // 2, p % 2
    gx, gzz = i // 8, i % 8
    gz, zl = gzz // 2, gzz % 2
    band = 4 * y + gz
    chip = 2 * gx + zl
    me = 2 * chip + core
    is_k = jnp.logical_and(core == 1, chip < HOLDERS)
    active = jnp.logical_or(i <= 8, i >= 24)
    lone = i == 8

    def dev(pp, ii):
        return {"band": pp, "fft": ii}

    def member(m):
        return dev(2 * y + m % 2, (m // 4) * 8 + 2 * gz + (m // 2) % 2)

    def holder(b, s):
        return dev(2 * (b // 4) + 1, (s // 2) * 8 + 2 * (b % 4) + s % 2)

    def remote(src, dst, ss, rs, where):
        return pltpu.make_async_remote_copy(
            src_ref=src, dst_ref=dst, send_sem=ss, recv_sem=rs, device_id=where, device_id_type=MESH
        )

    def await_bytes(ref, sem):
        pltpu.make_async_copy(ref, ref, sem).wait()

    lane = lax.broadcasted_iota(jnp.int32, (1, 128), 1)
    sign = jnp.where(lane < 64, -1.0, 1.0).astype(F32)

    def swap(x):
        return pltpu.roll(x, 64, 1)

    for k in range(6):
        xt[k] = xi_ref[k // 3, k % 3].T[:64]

    def kx_of(jj):
        return 3 * i + jj

    for k in range(6):
        j, jj = k // 3, k % 3
        b, kx = 2 * p + j, kx_of(jj)
        valid = jnp.logical_or(kx <= 24, kx >= 72)
        q = jnp.where(kx <= 24, kx, kx - 47)
        s, slot = (q // 8) % 8, q % 8
        s = jnp.minimum(s, HOLDERS - 1)
        target = holder(b, s)
        mine = jnp.logical_and(target["band"] == p, target["fft"] == i)

        @pl.when(jnp.logical_and(valid, mine))
        def _():
            pltpu.make_async_copy(xt.at[k], x0.at[slot], r_init.at[slot]).start()

        @pl.when(jnp.logical_and(valid, jnp.logical_not(mine)))
        def _():
            remote(xt.at[k], x0.at[slot], s_init.at[k], r_init.at[slot], target).start()

    vm, vhalf = i // 2, i % 2

    def v_target(n):
        g = 2 * core + n
        return dev(2 * y + vm % 2, (vm // 4) * 8 + 2 * g + (vm // 2) % 2)

    def v_mine(n):
        t = v_target(n)
        return jnp.logical_and(t["band"] == p, t["fft"] == i)

    for n in range(2):
        dst = vb.at[pl.ds(3 * vhalf, 3)]

        @pl.when(v_mine(n))
        def _():
            pltpu.make_async_copy(v_ref, dst, r_v.at[vhalf]).start()

        @pl.when(jnp.logical_not(v_mine(n)))
        def _():
            remote(v_ref, dst, s_v.at[n], r_v.at[vhalf], v_target(n)).start()

    @pl.when(is_k)
    def _():
        row = lax.broadcasted_iota(jnp.int32, (64, 128), 0)
        col_ = lax.broadcasted_iota(jnp.int32, (64, 128), 1) % 64
        fz = jnp.where(row <= 24, row, row - BOX)
        fy = jnp.where(col_ <= 24, col_, col_ - BOX)
        in_box = jnp.logical_and(row < BOX, col_ < BOX)
        yz = (fz * fz + fy * fy).astype(F32)
        absz = jnp.abs(fz).astype(F32)

        def plane(a, _):
            q = 8 * chip + a

            @pl.when(q < BOX)
            def _():
                await_bytes(x0.at[a], r_init.at[a])
                fx = jnp.where(q <= 24, q, q - BOX)
                data = x0[a]
                height = data[56:57]
                keep = jnp.logical_and(in_box, absz <= height)
                cur[a] = jnp.where(keep, data, 0.0)
                inside[a] = jnp.where(keep, 1.0 / CELLS, 0.0)
                kin[a] = jnp.where(keep, KIN * (yz + (fx * fx).astype(F32)), 0.0)

            @pl.when(q >= BOX)
            def _():
                zero = jnp.zeros((64, 128), F32)
                cur[a] = zero
                inside[a] = zero
                kin[a] = zero

            prev[a] = jnp.zeros((64, 128), F32)
            return 0

        lax.fori_loop(0, 8, plane, 0)

    for h in range(2):
        await_bytes(vb.at[pl.ds(3 * h, 3)], r_v.at[h])

    def forward():
        @pl.when(is_k)
        def _():
            x = jnp.concatenate([cur[a] for a in range(8)], axis=1)
            out = dot(ta_ref[...], pieces(x, 0))
            for a in range(8):
                c, s = out[:96, 128 * a : 128 * a + 128], out[96:, 128 * a : 128 * a + 128]
                sbuf[pl.ds(a, 96, stride=8), :] = c + sign * swap(s)

            def send(m, _):
                src = sbuf.at[pl.ds(pl.multiple_of(48 * m, 8), 48)]

                @pl.when(m == me)
                def _():
                    pltpu.make_async_copy(src, rbuf.at[chip], r_f.at[chip]).start()

                @pl.when(m != me)
                def _():
                    remote(src, rbuf.at[chip], s_f.at[m], r_f.at[chip], member(m)).start()

                return 0

            lax.fori_loop(0, MEMBERS, send, 0)

    def middle():
        for s in range(HOLDERS):
            await_bytes(rbuf.at[s], r_f.at[s])
        zero8 = jnp.zeros((8, 128), F32)
        d = jnp.concatenate(
            [
                jnp.concatenate([rbuf[s, 8 * z : 8 * z + 8, :] for s in range(HOLDERS)] + [zero8], axis=0)
                for z in range(ZP)
            ],
            axis=1,
        )
        out = dot(ta_ref[...], pieces(d, 0))
        planes = [
            out[:96, 128 * z : 128 * z + 128] + sign * swap(out[96:, 128 * z : 128 * z + 128])
            for z in range(ZP)
        ]
        for z in range(ZP):
            psi = dot(pieces(planes[z], 1), ty_ref[...])
            v = vb[z]
            psi = psi * jnp.concatenate([v, v], axis=1)
            planes[z] = dot(pieces(psi, 1), tyb_ref[...])
        out = dot(tb_ref[...], pieces(jnp.concatenate(planes, axis=1), 0))
        for z in range(ZP):
            o = out[:64, 128 * z : 128 * z + 128] - sign * swap(out[64:, 128 * z : 128 * z + 128])
            for s in range(HOLDERS):
                bbuf[s, 8 * z : 8 * z + 8, :] = o[8 * s : 8 * s + 8]

        def send(s, _):
            home = pl.ds(pl.multiple_of(48 * me, 8), 48)
            mine = jnp.logical_and(is_k, s == chip)

            @pl.when(mine)
            def _():
                pltpu.make_async_copy(bbuf.at[s], kbuf.at[home], r_b.at[me]).start()

            @pl.when(jnp.logical_not(mine))
            def _():
                remote(bbuf.at[s], kbuf.at[home], s_b.at[s], r_b.at[me], holder(band, s)).start()

            return 0

        lax.fori_loop(0, HOLDERS, send, 0)

    def backward(finish):
        @pl.when(is_k)
        def _():
            def arrive(m, _):
                await_bytes(kbuf.at[pl.ds(pl.multiple_of(48 * m, 8), 48)], r_b.at[m])
                return 0

            lax.fori_loop(0, MEMBERS, arrive, 0)
            d = jnp.concatenate([kbuf[pl.ds(a, 96, stride=8), :] for a in range(8)], axis=1)
            out = dot(tb_ref[...], pieces(d, 0))
            for a in range(8):
                f = out[:64, 128 * a : 128 * a + 128] - sign * swap(out[64:, 128 * a : 128 * a + 128])
                finish(a, kin[a] * cur[a] + inside[a] * f)

            def sent(m, _):
                @pl.when(m != me)
                def _():
                    await_bytes(sbuf.at[pl.ds(pl.multiple_of(48 * m, 8), 48)], s_f.at[m])

                return 0

            lax.fori_loop(0, MEMBERS, sent, 0)

        def sent_back(s, _):
            @pl.when(jnp.logical_not(jnp.logical_and(is_k, s == chip)))
            def _():
                await_bytes(bbuf.at[s], s_b.at[s])

            return 0

        lax.fori_loop(0, HOLDERS, sent_back, 0)

    center = 0.5 * (upper_ref[0] + lower_ref[0])
    half_width = 0.5 * (upper_ref[0] - lower_ref[0])

    def step(k, _):
        forward()
        middle()
        alpha = jnp.where(k == 0, 1.0, 2.0).astype(F32)
        beta = jnp.where(k == 0, 0.0, 1.0).astype(F32)

        def finish(a, h):
            old = cur[a]
            new = alpha * (h - center * old) / half_width - beta * prev[a]
            prev[a] = old
            cur[a] = new

        backward(finish)
        return 0

    lax.fori_loop(0, 3, step, 0)

    n_planes = jnp.where(chip == HOLDERS - 1, 1, 8)

    def scatter(src, w):
        @pl.when(is_k)
        def _():
            def one(n, _):
                a, t = n // 7, n % 7
                q = 8 * chip + a
                kx = jnp.where(q <= 24, q, q + 47)
                dst = gy.at[w, pl.ds(pl.multiple_of(128 * (kx % 3) + 8 * band, 8), 8)]
                row = src.at[a, pl.ds(pl.multiple_of(8 * t, 8), 8)]
                ii = kx // 3
                mine = jnp.logical_and(t == p, ii == i)

                @pl.when(mine)
                def _():
                    pltpu.make_async_copy(row, dst, r_g.at[w, kx % 3, band]).start()

                @pl.when(jnp.logical_not(mine))
                def _():
                    remote(row, dst, s_g.at[w, n], r_g.at[w, kx % 3, band], dev(t, ii)).start()

                return 0

            lax.fori_loop(0, 7 * n_planes, one, 0)

    def scattered(src, w):
        @pl.when(is_k)
        def _():
            def one(n, _):
                a, t = n // 7, n % 7
                q = 8 * chip + a
                kx = jnp.where(q <= 24, q, q + 47)

                @pl.when(jnp.logical_not(jnp.logical_and(t == p, kx // 3 == i)))
                def _():
                    await_bytes(src.at[a, pl.ds(pl.multiple_of(8 * t, 8), 8)], s_g.at[w, n])

                return 0

            lax.fori_loop(0, 7 * n_planes, one, 0)

    summing = jnp.logical_and(active, p < 7)

    def gather_wait(w):
        def one(n, _):
            jj, b = n // BANDS, n % BANDS
            await_bytes(gy.at[w, pl.ds(pl.multiple_of(128 * jj + 8 * b, 8), 8)], r_g.at[w, jj, b])
            return 0

        lax.fori_loop(0, jnp.where(lone, BANDS, 3 * BANDS), one, 0)

    def rows_of(w):
        out = []
        for jj in range(3):
            for r in range(8):
                x = gy[w, pl.ds(128 * jj + r, BANDS, stride=8), :]
                if jj:
                    x = jnp.where(lone, 0.0, x)
                out.append(x)
        return out

    def with_swapped(rows):
        a = jnp.concatenate(rows, axis=1)
        b = jnp.concatenate([-sign * swap(x) for x in rows], axis=1)
        return jnp.concatenate([a, b], axis=0)

    def partial_sum(w):
        @pl.when(summing)
        def _():
            gather_wait(w)
            high, low = split(with_swapped(rows_of(w)))
            if w == 0:
                bh[...] = high
                bl[...] = low
            g = (
                dot_t(bh[:BANDS], high)
                + dot_t(bh[:BANDS], low)
                + dot_t(bl[:BANDS], high)
            ) * (1.0 / CELLS)
            g = jnp.concatenate([g, jnp.zeros((BANDS, 96), F32)], axis=1)
            part[w] = g
            col[w, p] = g

            def send(t, _):
                @pl.when(t != p)
                def _():
                    remote(part.at[w], col.at[w, p], s_c.at[w, t], r_c.at[w, p], dev(t, i)).start()

                return 0

            lax.fori_loop(0, 8, send, 0)

    slot = jnp.where(i <= 8, i, i - 15)

    def column_sum(w):
        @pl.when(active)
        def _():
            def arrive(t, _):
                @pl.when(t != p)
                def _():
                    await_bytes(col.at[w, t], r_c.at[w, t])

                return 0

            lax.fori_loop(0, 7, arrive, 0)
            total = col[w, 0]
            for t in range(1, 7):
                total = total + col[w, t]
            csum[w] = total
            my_slot = jnp.minimum(jnp.maximum(slot, 0), 16)
            full[w, my_slot] = total

            def send(ii, _):
                @pl.when(ii != i)
                def _():
                    remote(
                        csum.at[w], full.at[w, my_slot], s_p.at[w, ii], r_p.at[w, my_slot], dev(p, ii)
                    ).start()

                return 0

            lax.fori_loop(0, 32, send, 0)

    def total_of(w):
        def arrive(n, _):
            @pl.when(jnp.where(n <= 8, n, n + 15) != i)
            def _():
                await_bytes(full.at[w, n], r_p.at[w, n])

            return 0

        lax.fori_loop(0, 17, arrive, 0)
        total = full[w, 0]
        for n in range(1, 17):
            total = total + full[w, n]
        return total

    lane2 = lax.broadcasted_iota(jnp.int32, (16, 128), 1)

    def embed(g):
        top = jnp.where(lane2 < 16, g, -g)
        bottom = jnp.where(lane2 < 16, pltpu.roll(g, 112, 1), pltpu.roll(g, 16, 1))
        return jnp.where(jnp.concatenate([lane2, lane2], 0) < 32, jnp.concatenate([top, bottom], 0), 0.0)

    def inverse_rows(g):
        row = lax.broadcasted_iota(jnp.int32, (32, 128), 0)
        ln = lax.broadcasted_iota(jnp.int32, (32, 128), 1)
        m = embed(g) + jnp.where(ln == row + 32, 1.0, 0.0)
        for j in range(32):
            pivot = m[j : j + 1, :]
            factor = m[:, j : j + 1] * (1.0 / pivot[:, j : j + 1])
            m = m - jnp.where(row > j, factor, 0.0) * pivot
        diag = jnp.sum(jnp.where(ln == row, m, 0.0), axis=1, keepdims=True)
        u = m[:16] / jnp.sqrt(diag[:16])
        return jnp.where(lane2 < 32, pltpu.roll(u, 96, 1), 0.0)

    scatter(cur, 0)
    forward()
    middle()
    partial_sum(0)

    def keep(a, h):
        hy[a] = h

    backward(keep)
    scatter(hy, 1)
    column_sum(0)
    u = inverse_rows(total_of(0))

    @pl.when(summing)
    def _():
        w2 = jnp.where(lane2 < 16, u, -u)[:, :32]
        w_high, w_low = split(w2)
        q = dot(w_high, bh[...]) + dot(w_high, bl[...]) + dot(w_low, bh[...])
        for n in range(24):
            qs[pl.ds(n, BANDS, stride=24), :] = q[:, 128 * n : 128 * n + 128]

        def send(t, _):
            src = qs.at[pl.ds(pl.multiple_of(48 * t, 8), 48)]

            @pl.when(t == p)
            def _():
                pltpu.make_async_copy(src, ob.at[p], r_o.at[p]).start()

            @pl.when(t != p)
            def _():
                remote(src, ob.at[p], s_o.at[t], r_o.at[p], dev(t, i)).start()

            return 0

        lax.fori_loop(0, 8, send, 0)

    partial_sum(1)
    column_sum(1)

    @pl.when(active)
    def _():
        for t in range(7):
            await_bytes(ob.at[t], r_o.at[t])
        zero = jnp.zeros((72, 128), F32)
        for k in range(6):
            plane = jnp.concatenate([ob[t, 8 * k : 8 * k + 8, :] for t in range(7)] + [zero], axis=0)
            if k % 3:
                plane = jnp.where(lone, 0.0, plane)
            out_ref[k // 3, k % 3] = plane.T

    @pl.when(jnp.logical_not(active))
    def _():
        out_ref[...] = jnp.zeros((2, 3, 128, 128), F32)

    h = embed(total_of(1))
    t = jnp.dot(u[:, :32], h, precision=lax.Precision.HIGHEST, preferred_element_type=F32)
    energy_ref[...] = jnp.broadcast_to(jnp.sum(t * u, axis=1, keepdims=True), (16, 128))

    for k in range(6):
        j, jj = k // 3, k % 3
        kx = kx_of(jj)
        valid = jnp.logical_or(kx <= 24, kx >= 72)
        q = jnp.where(kx <= 24, kx, kx - 47)
        s = jnp.minimum((q // 8) % 8, HOLDERS - 1)
        target = holder(2 * p + j, s)
        mine = jnp.logical_and(target["band"] == p, target["fft"] == i)

        @pl.when(jnp.logical_and(valid, jnp.logical_not(mine)))
        def _():
            await_bytes(xt.at[k], s_init.at[k])

    for n in range(2):

        @pl.when(jnp.logical_not(v_mine(n)))
        def _():
            await_bytes(v_ref, s_v.at[n])

    scattered(cur, 0)
    scattered(hy, 1)
    for w in range(2):

        @pl.when(summing)
        def _():
            def sent(t, _):
                @pl.when(t != p)
                def _():
                    await_bytes(part.at[w], s_c.at[w, t])

                return 0

            lax.fori_loop(0, 8, sent, 0)

        @pl.when(active)
        def _():
            def sent(ii, _):
                @pl.when(ii != i)
                def _():
                    await_bytes(csum.at[w], s_p.at[w, ii])

                return 0

            lax.fori_loop(0, 32, sent, 0)

    @pl.when(summing)
    def _():
        def sent(t, _):
            @pl.when(t != p)
            def _():
                await_bytes(qs.at[pl.ds(pl.multiple_of(48 * t, 8), 48)], s_o.at[t])

            return 0

        lax.fori_loop(0, 8, sent, 0)


def call(lower, upper, xi, v):
    vmem = pl.BlockSpec(memory_space=pltpu.VMEM)
    smem = pl.BlockSpec(memory_space=pltpu.SMEM)
    sem = pltpu.SemaphoreType.DMA

    def buf(*shape):
        return pltpu.VMEM(shape, F32)

    return pl.pallas_call(
        kernel,
        out_shape=(
            jax.ShapeDtypeStruct((2, 3, 128, 128), F32),
            jax.ShapeDtypeStruct((16, 128), F32),
        ),
        in_specs=[smem, smem] + [vmem] * 6,
        out_specs=(vmem, vmem),
        scratch_shapes=[
            buf(6, 64, 128),
            buf(8, 64, 128),
            buf(6, 96, 128),
            buf(8, 64, 128),
            buf(8, 64, 128),
            buf(8, 64, 128),
            buf(8, 64, 128),
            buf(8, 64, 128),
            buf(768, 128),
            buf(7, 48, 128),
            buf(7, 48, 128),
            buf(768, 128),
            buf(2, 384, 128),
            pltpu.VMEM((32, 3072), BF16),
            pltpu.VMEM((32, 3072), BF16),
            buf(2, 16, 128),
            buf(2, 8, 16, 128),
            buf(2, 16, 128),
            buf(2, 17, 16, 128),
            buf(384, 128),
            buf(7, 48, 128),
            sem((6,)),
            sem((8,)),
            sem((2,)),
            sem((2,)),
            sem((16,)),
            sem((7,)),
            sem((7,)),
            sem((16,)),
            sem((2, 56)),
            sem((2, 3, 16)),
            sem((2, 8)),
            sem((2, 8)),
            sem((2, 32)),
            sem((2, 17)),
            sem((8,)),
            sem((7,)),
        ],
        compiler_params=pltpu.CompilerParams(has_side_effects=True, vmem_limit_bytes=48 * 2**20),
    )(lower, upper, xi, v, *[jnp.asarray(t) for t in tables()])


def boxed(x, axis):
    index = [slice(None)] * x.ndim
    index[axis] = slice(0, 25)
    low = x[tuple(index)]
    index[axis] = slice(72, 96)
    return jnp.concatenate([low, x[tuple(index)]], axis=axis)


def unboxed(x, axis):
    index = [slice(None)] * x.ndim
    index[axis] = slice(0, 25)
    low = x[tuple(index)]
    index[axis] = slice(25, 49)
    high = x[tuple(index)]
    shape = list(x.shape)
    shape[axis] = 47
    return jnp.concatenate([low, jnp.zeros(shape, x.dtype), high], axis=axis)


def local(start_bands, potential, half_height, lower_bound, upper_bound, fermi_level):
    x = start_bands.reshape(2, 2, 3, NG, NG)
    x = boxed(boxed(x, 3), 4)
    x = jnp.pad(x, ((0, 0), (0, 0), (0, 0), (0, 15), (0, 7)))
    height = jnp.pad(boxed(half_height, 1), ((0, 0), (0, 15)), constant_values=-1).astype(F32)
    height = jnp.broadcast_to(height[None, None, :, :, None], (2, 2, 3, 64, 1))
    x = jnp.concatenate([x, height, jnp.zeros((2, 2, 3, 64, 71), F32)], axis=4)
    xi = x.transpose(1, 2, 0, 3, 4).reshape(2, 3, 128, 128)
    v = jnp.pad(potential.transpose(2, 0, 1), ((0, 0), (0, 0), (0, 32)))
    out, energy = call(lower_bound, upper_bound, xi, v)
    q = out.reshape(2, 3, 2, 64, 128)[:, :, :, :BOX, :BOX].transpose(2, 0, 1, 3, 4)
    bands = unboxed(unboxed(q, 3), 4).reshape(2, 2, 3, NG * NG)
    energies = energy[:, 0]
    own = lax.dynamic_slice_in_dim(energies, 2 * lax.axis_index("band"), 2, 0)
    weights = jax.nn.sigmoid((fermi_level[0] - energies) / TEMPER)
    band_energy = (jnp.sum(weights * energies) / float(BANDS)).reshape(1)
    return bands, own, band_energy


def solution(mesh):
    placed = (P(None, "band", "fft", None), P(None, None, "fft"), P("fft", None), P(), P(), P())
    return jax.shard_map(
        local,
        mesh=mesh,
        in_specs=placed,
        out_specs=(P(None, "band", "fft", None), P("band"), P()),
        check_vma=False,
    )
```

```python
import math

import jax
import jax.numpy as jnp
import ml_dtypes
import numpy as np
from jax import lax
from jax.experimental import pallas as pl
from jax.experimental.pallas import tpu as pltpu
from jax.sharding import PartitionSpec as P

NG = 96
CELLS = float(NG**3)
BOX = 49
KIN = 12.0 / 24**2
TEMPER = 0.5
BANDS = 16
MEMBERS = 16
HOLDERS = 7
ZP = 3
F32, BF16 = jnp.float32, jnp.bfloat16
MESH = pl.DeviceIdType.MESH


def box_frequency():
    r = np.arange(BOX)
    return np.where(r <= 24, r, r - BOX)


def halves(table):
    table = table.astype(np.float32)
    high = table.astype(ml_dtypes.bfloat16)
    low = (table - high.astype(np.float32)).astype(ml_dtypes.bfloat16)
    return high, low


def tables():
    freq = box_frequency()
    angle = 2.0 * math.pi / NG * ((np.arange(NG)[:, None] * freq[None, :]) % NG)
    cosine, sine = np.cos(angle), np.sin(angle)
    ahead = np.zeros((192, 64))
    ahead[:96, :BOX], ahead[96:, :BOX] = cosine, sine
    back = np.zeros((128, 96))
    back[:BOX], back[64 : 64 + BOX] = cosine.T, sine.T
    lanes = np.zeros((128, 256))
    lanes[:BOX, :96], lanes[:BOX, 128:224] = cosine.T, sine.T
    lanes[64 : 64 + BOX, :96], lanes[64 : 64 + BOX, 128:224] = -sine.T, cosine.T
    lanes_back = lanes.T.copy()
    plane = np.arange(NG).reshape(MEMBERS, 2, ZP)

    def left(t):
        high, low = halves(t)
        return np.concatenate([high, high, low], axis=1)

    def right(t):
        high, low = halves(t)
        return np.concatenate([high, high, low], axis=0)

    z_ahead = [np.concatenate([ahead[plane[:, h].ravel()], ahead[96 + plane[:, h].ravel()]]) for h in range(2)]
    z_back = [back[:, plane[:, h].ravel()] for h in range(2)]
    return (
        np.stack([left(t) for t in z_ahead]),
        left(ahead),
        np.stack([left(t) for t in z_back]),
        left(back),
        right(lanes),
        right(lanes_back),
    )


def split(x):
    high = x.astype(BF16)
    return high, (x - high.astype(F32)).astype(BF16)


def pieces(x, axis):
    high, low = split(x)
    return jnp.concatenate([high, low, high], axis=axis)


def dot(a, b):
    return jnp.dot(a, b, preferred_element_type=F32)


def dot_t(a, b):
    return lax.dot_general(a, b, (((1,), (1,)), ((), ())), preferred_element_type=F32)


def kernel(
    lower_ref,
    upper_ref,
    fermi_ref,
    height_ref,
    x_hbm,
    v_hbm,
    tz_hbm,
    tx_hbm,
    tzb_hbm,
    txb_hbm,
    ty_hbm,
    tyb_hbm,
    out_hbm,
    energy_ref,
    band_energy_ref,
    xin,
    grid,
    tz,
    tx,
    tzb,
    txb,
    ty,
    tyb,
    xt,
    x0,
    vb,
    cur,
    prev,
    hy,
    inside,
    kin,
    sbuf,
    rbuf,
    bbuf,
    kbuf,
    gy,
    bh,
    bl,
    part,
    col,
    csum,
    full,
    epart,
    ecol,
    ecsum,
    efull,
    qs,
    ob,
    s_in,
    s_out,
    s_t,
    s_init,
    r_init,
    s_v,
    r_v,
    s_f,
    r_f,
    s_b,
    r_b,
    s_g,
    r_g,
    s_c,
    r_c,
    s_p,
    r_p,
    s_o,
    r_o,
    planes_in,
):
    p = lax.axis_index("band")
    i = lax.axis_index("fft")
    y, core = p // 2, p % 2
    y2, yl = y // 2, y % 2
    gx, gzz = i // 8, i % 8
    x2, xl = gx // 2, gx % 2
    gz, zl = gzz // 2, gzz % 2
    band = 8 * y2 + 4 * x2 + gz
    chip = 4 * yl + 2 * xl + zl
    me = 2 * chip + core
    is_k = jnp.logical_and(core == 1, chip < HOLDERS)
    active = jnp.logical_or(i <= 8, i >= 24)
    lone = i == 8
    summing = jnp.logical_and(active, p < 7)

    def dev(pp, ii):
        return {"band": pp, "fft": ii}

    def member_of(b, m):
        c = m // 2
        return dev(
            2 * (2 * (b // 8) + c // 4) + m % 2,
            (2 * ((b // 4) % 2) + (c // 2) % 2) * 8 + 2 * (b % 4) + c % 2,
        )

    def holder(b, s):
        return member_of(b, 2 * s + 1)

    def is_me(where):
        return jnp.logical_and(where["band"] == p, where["fft"] == i)

    def remote(src, dst, ss, rs, where):
        return pltpu.make_async_remote_copy(
            src_ref=src, dst_ref=dst, send_sem=ss, recv_sem=rs, device_id=where, device_id_type=MESH
        )

    def await_bytes(ref, sem):
        pltpu.make_async_copy(ref, ref, sem).wait()

    barrier = pltpu.get_barrier_semaphore()
    here = (p % 4) * 32 + i

    def greet(n, _):
        at = (here + n) % 128
        pl.semaphore_signal(barrier, inc=1, device_id=dev(4 * (p // 4) + at // 32, at % 32), device_id_type=MESH)
        return 0

    def others(n):
        return dev(4 * (1 - p // 4) + n, i)

    pltpu.make_async_copy(x_hbm, xin, s_in.at[0]).start()
    for n, (src, dst) in enumerate(
        ((tz_hbm, tz), (tx_hbm, tx), (tzb_hbm, tzb), (txb_hbm, txb), (ty_hbm, ty), (tyb_hbm, tyb))
    ):
        pltpu.make_async_copy(src, dst, s_t.at[n]).start()
    lax.fori_loop(1, 128, greet, 0)
    for n in range(4):
        pl.semaphore_signal(barrier, inc=1, device_id=others(n), device_id_type=MESH)

    lane = lax.broadcasted_iota(jnp.int32, (1, 128), 1)
    sign = jnp.where(lane < 64, -1.0, 1.0).astype(F32)

    def swap(x):
        return pltpu.roll(x, 64, 1)

    def boxed_lanes(x):
        return jnp.where(lane < 25, x, jnp.where(lane < BOX, pltpu.roll(x, 128 - 47, 1), 0.0))

    await_bytes(xin, s_in.at[0])
    for k in range(6):
        j, jj = k // 3, k % 3
        for c in range(2):
            t0, t1, t2 = (xin[3 * c + jj, pl.ds(2 * t + j, 24, stride=6), :] for t in range(3))
            quarter = (
                t0,
                jnp.where(lane < 32, pltpu.roll(t0, 32, 1), pltpu.roll(t1, 32, 1)),
                jnp.where(lane < 64, pltpu.roll(t1, 64, 1), pltpu.roll(t2, 64, 1)),
                pltpu.roll(t2, 96, 1),
            )
            for r in range(4):
                grid[c, pl.ds(r, 24, stride=4), :] = boxed_lanes(quarter[r])
        pad = jnp.zeros((15, 128), F32)
        rows = jnp.concatenate([grid[0, 0:25], grid[0, 72:96], pad, grid[1, 0:25], grid[1, 72:96], pad], axis=0)
        xt[k] = rows.T[:64]
    for jj in range(3):
        h = height_ref[jj : jj + 1, :].astype(F32)
        h = boxed_lanes(jnp.concatenate([h, jnp.zeros((1, 32), F32)], axis=1))
        h = jnp.where(lane < BOX, h, -1.0)
        h = jnp.where(lane < 64, h, pltpu.roll(h, 64, 1))
        for j in range(2):
            xt[3 * j + jj, 56:57, :] = h

    pl.semaphore_wait(barrier, 131)
    for n in range(4):
        pl.semaphore_signal(planes_in, inc=1, device_id=others(n), device_id_type=MESH)

    def start_of(k):
        j, jj = k // 3, k % 3
        kx = 3 * i + jj
        valid = jnp.logical_or(kx <= 24, kx >= 72)
        q = jnp.where(kx <= 24, kx, kx - 47)
        s = jnp.minimum((q // 8) % 8, HOLDERS - 1)
        return valid, q % 8, holder(2 * p + j, s)

    for k in range(6):
        valid, slot, target = start_of(k)

        @pl.when(jnp.logical_and(valid, is_me(target)))
        def _():
            pltpu.make_async_copy(xt.at[k], x0.at[slot], r_init.at[slot]).start()

        @pl.when(jnp.logical_and(valid, jnp.logical_not(is_me(target))))
        def _():
            remote(xt.at[k], x0.at[slot], s_init.at[k], r_init.at[slot], target).start()

    gives_v = jnp.logical_and(core == 0, yl == i // 16)

    @pl.when(gives_v)
    def _():
        def one(g, _):
            target = member_of(8 * y2 + g, i // 2)
            dst = vb.at[pl.ds(3 * (i % 2), 3)]

            @pl.when(is_me(target))
            def _():
                pltpu.make_async_copy(v_hbm, dst, r_v.at[i % 2]).start()

            @pl.when(jnp.logical_not(is_me(target)))
            def _():
                remote(v_hbm, dst, s_v.at[g], r_v.at[i % 2], target).start()

            return 0

        lax.fori_loop(0, 8, one, 0)

    for n, dst in enumerate((tz, tx, tzb, txb, ty, tyb)):
        await_bytes(dst, s_t.at[n])

    @pl.when(is_k)
    def _():
        row = lax.broadcasted_iota(jnp.int32, (64, 128), 0)
        col_ = lax.broadcasted_iota(jnp.int32, (64, 128), 1) % 64
        fz = jnp.where(row <= 24, row, row - BOX)
        fy = jnp.where(col_ <= 24, col_, col_ - BOX)
        in_box = jnp.logical_and(row < BOX, col_ < BOX)
        yz = (fz * fz + fy * fy).astype(F32)
        absz = jnp.abs(fz).astype(F32)

        def plane(a, _):
            q = 8 * chip + a

            @pl.when(q < BOX)
            def _():
                await_bytes(x0.at[a], r_init.at[a])
                fx = jnp.where(q <= 24, q, q - BOX)
                data = x0[a]
                height = data[56:57]
                keep = jnp.logical_and(in_box, absz <= height)
                cur[a] = jnp.where(keep, data, 0.0)
                inside[a] = jnp.where(keep, 1.0 / CELLS, 0.0)
                kin[a] = jnp.where(keep, KIN * (yz + (fx * fx).astype(F32)), 0.0)

            @pl.when(q >= BOX)
            def _():
                zero = jnp.zeros((64, 128), F32)
                cur[a] = zero
                inside[a] = zero
                kin[a] = zero

            prev[a] = jnp.zeros((64, 128), F32)
            return 0

        lax.fori_loop(0, 8, plane, 0)

    def message(m):
        return pl.ds(pl.multiple_of(24 * m, 8), 24)

    def forward():
        @pl.when(is_k)
        def _():
            x = pieces(jnp.concatenate([cur[a] for a in range(8)], axis=1), 0)
            for h in range(2):
                out = dot(tz[h], x)
                for a in range(8):
                    c, s = out[:48, 128 * a : 128 * a + 128], out[48:, 128 * a : 128 * a + 128]
                    sbuf[h, pl.ds(a, 48, stride=8), :] = c + sign * swap(s)

                def send(m, _):
                    src = sbuf.at[h, message(m)]

                    @pl.when(m == me)
                    def _():
                        pltpu.make_async_copy(src, rbuf.at[h, chip], r_f.at[h, chip]).start()

                    @pl.when(m != me)
                    def _():
                        remote(
                            src, rbuf.at[h, chip], s_f.at[h, m], r_f.at[h, chip], member_of(band, m)
                        ).start()

                    return 0

                lax.fori_loop(0, MEMBERS, send, 0)

    def middle(first):
        zero8 = jnp.zeros((8, 128), F32)
        zero32 = jnp.zeros((288, 32), F32)
        for h in range(2):
            for s in range(HOLDERS):
                await_bytes(rbuf.at[h, s], r_f.at[h, s])
            d = jnp.concatenate(
                [
                    jnp.concatenate(
                        [rbuf[h, s, 8 * z : 8 * z + 8, :] for s in range(HOLDERS)] + [zero8], axis=0
                    )
                    for z in range(ZP)
                ],
                axis=1,
            )
            out = dot(tx[...], pieces(d, 0))
            rows = jnp.concatenate(
                [
                    out[:96, 128 * z : 128 * z + 128] + sign * swap(out[96:, 128 * z : 128 * z + 128])
                    for z in range(ZP)
                ],
                axis=0,
            )
            psi = dot(pieces(rows, 1), ty[...])

            @pl.when(first)
            def _():
                await_bytes(vb.at[pl.ds(3 * h, 3)], r_v.at[h])

            v = jnp.concatenate([vb[3 * h + z] for z in range(ZP)], axis=0)
            v = jnp.concatenate([v, zero32], axis=1)
            psi = psi * jnp.concatenate([v, v], axis=1)
            rows = dot(pieces(psi, 1), tyb[...])
            d = jnp.concatenate([rows[96 * z : 96 * z + 96] for z in range(ZP)], axis=1)
            out = dot(txb[...], pieces(d, 0))
            for z in range(ZP):
                o = out[:64, 128 * z : 128 * z + 128] - sign * swap(out[64:, 128 * z : 128 * z + 128])
                for s in range(HOLDERS):
                    bbuf[h, s, 8 * z : 8 * z + 8, :] = o[8 * s : 8 * s + 8]

            def send(s, _):
                home = kbuf.at[h, message(me)]
                mine = jnp.logical_and(is_k, s == chip)

                @pl.when(mine)
                def _():
                    pltpu.make_async_copy(bbuf.at[h, s], home, r_b.at[h, me]).start()

                @pl.when(jnp.logical_not(mine))
                def _():
                    remote(bbuf.at[h, s], home, s_b.at[h, s], r_b.at[h, me], holder(band, s)).start()

                return 0

            lax.fori_loop(0, HOLDERS, send, 0)

    def backward(finish):
        @pl.when(is_k)
        def _():
            out = None
            for h in range(2):

                def arrive(m, _):
                    await_bytes(kbuf.at[h, message(m)], r_b.at[h, m])
                    return 0

                lax.fori_loop(0, MEMBERS, arrive, 0)
                d = jnp.concatenate([kbuf[h, pl.ds(a, 48, stride=8), :] for a in range(8)], axis=1)
                term = dot(tzb[h], pieces(d, 0))
                out = term if out is None else out + term
            for a in range(8):
                f = out[:64, 128 * a : 128 * a + 128] - sign * swap(out[64:, 128 * a : 128 * a + 128])
                finish(a, kin[a] * cur[a] + inside[a] * f)

            for h in range(2):

                def sent(m, _):
                    @pl.when(m != me)
                    def _():
                        await_bytes(sbuf.at[h, message(m)], s_f.at[h, m])

                    return 0

                lax.fori_loop(0, MEMBERS, sent, 0)

        for h in range(2):

            def sent_back(s, _):
                @pl.when(jnp.logical_not(jnp.logical_and(is_k, s == chip)))
                def _():
                    await_bytes(bbuf.at[h, s], s_b.at[h, s])

                return 0

            lax.fori_loop(0, HOLDERS, sent_back, 0)

    center = 0.5 * (upper_ref[0] + lower_ref[0])
    half_width = 0.5 * (upper_ref[0] - lower_ref[0])

    def step(k, _):
        forward()
        middle(k == 0)
        alpha = jnp.where(k == 0, 1.0, 2.0).astype(F32)
        beta = jnp.where(k == 0, 0.0, 1.0).astype(F32)

        def finish(a, h):
            old = cur[a]
            new = alpha * (h - center * old) / half_width - beta * prev[a]
            prev[a] = old
            cur[a] = new

        backward(finish)
        return 0

    lax.fori_loop(0, 3, step, 0)

    n_planes = jnp.where(chip == HOLDERS - 1, 1, 8)

    def row_of(n):
        a, t = n // 7, n % 7
        q = 8 * chip + a
        return a, t, jnp.where(q <= 24, q, q + 47)

    def scatter(src, w):
        @pl.when(is_k)
        def _():
            def one(n, _):
                a, t, kx = row_of(n)
                dst = gy.at[w, pl.ds(pl.multiple_of(128 * (kx % 3) + 8 * band, 8), 8)]
                row = src.at[a, pl.ds(pl.multiple_of(8 * t, 8), 8)]
                target = dev(t, kx // 3)

                @pl.when(is_me(target))
                def _():
                    pltpu.make_async_copy(row, dst, r_g.at[w, kx % 3, band]).start()

                @pl.when(jnp.logical_not(is_me(target)))
                def _():
                    remote(row, dst, s_g.at[w, n], r_g.at[w, kx % 3, band], target).start()

                return 0

            lax.fori_loop(0, 7 * n_planes, one, 0)

    def scattered(src, w):
        @pl.when(is_k)
        def _():
            def one(n, _):
                a, t, kx = row_of(n)

                @pl.when(jnp.logical_not(is_me(dev(t, kx // 3))))
                def _():
                    await_bytes(src.at[a, pl.ds(pl.multiple_of(8 * t, 8), 8)], s_g.at[w, n])

                return 0

            lax.fori_loop(0, 7 * n_planes, one, 0)

    def all_rows(w):
        def one(n, _):
            jj, b = n // BANDS, n % BANDS
            await_bytes(gy.at[w, pl.ds(pl.multiple_of(128 * jj + 8 * b, 8), 8)], r_g.at[w, jj, b])
            return 0

        lax.fori_loop(0, jnp.where(lone, BANDS, 3 * BANDS), one, 0)
        rows = []
        for jj in range(3):
            for r in range(8):
                x = gy[w, pl.ds(128 * jj + r, BANDS, stride=8), :]
                rows.append(jnp.where(lone, 0.0, x) if jj else x)
        a = jnp.concatenate(rows, axis=1)
        b = jnp.concatenate([-sign * swap(x) for x in rows], axis=1)
        return jnp.concatenate([a, b], axis=0)

    my_slot = jnp.minimum(jnp.where(i <= 8, i, jnp.maximum(i - 15, 0)), 16)

    def slot_fft(n):
        return jnp.where(n <= 8, n, n + 15)

    def column_send(w, mine, theirs):
        def send(t, _):
            @pl.when(t != p)
            def _():
                remote(mine, theirs.at[p], s_c.at[w, t], r_c.at[w, p], dev(t, i)).start()

            return 0

        lax.fori_loop(0, 8, send, 0)

    def column_sum(w, theirs):
        def arrive(t, _):
            @pl.when(t != p)
            def _():
                await_bytes(theirs.at[t], r_c.at[w, t])

            return 0

        lax.fori_loop(0, 7, arrive, 0)
        total = theirs[0]
        for t in range(1, 7):
            total = total + theirs[t]
        return total

    def plane_send(w, mine, theirs, count, fft_of):
        def send(n, _):
            ii = fft_of(n)

            @pl.when(ii != i)
            def _():
                remote(mine, theirs.at[my_slot], s_p.at[w, n], r_p.at[w, my_slot], dev(p, ii)).start()

            return 0

        lax.fori_loop(0, count, send, 0)

    def plane_sum(w, theirs):
        def arrive(n, _):
            @pl.when(slot_fft(n) != i)
            def _():
                await_bytes(theirs.at[n], r_p.at[w, n])

            return 0

        lax.fori_loop(0, 17, arrive, 0)
        total = theirs[0]
        for n in range(1, 17):
            total = total + theirs[n]
        return total

    lane2 = lax.broadcasted_iota(jnp.int32, (16, 128), 1)

    def inverse_rows(g):
        row = lax.broadcasted_iota(jnp.int32, (32, 128), 0)
        ln = lax.broadcasted_iota(jnp.int32, (32, 128), 1)
        top = jnp.where(lane2 < 16, g, -g)
        bottom = jnp.where(lane2 < 16, pltpu.roll(g, 112, 1), pltpu.roll(g, 16, 1))
        m = jnp.where(ln < 32, jnp.concatenate([top, bottom], 0), 0.0)
        m = m + jnp.where(ln == row + 32, 1.0, 0.0)
        for j in range(32):
            pivot = m[j : j + 1, :]
            factor = m[:, j : j + 1] * (1.0 / pivot[:, j : j + 1])
            m = m - jnp.where(row > j, factor, 0.0) * pivot
        diag = jnp.sum(jnp.where(ln == row, m, 0.0), axis=1, keepdims=True)
        u = m[:16] / jnp.sqrt(diag[:16])
        return jnp.where(lane2 < 32, pltpu.roll(u, 96, 1), 0.0)

    forward()
    pl.semaphore_wait(planes_in, 4)
    scatter(cur, 0)
    middle(False)

    @pl.when(summing)
    def _():
        high, low = split(all_rows(0))
        bh[...] = high
        bl[...] = low
        g = (dot_t(bh[:BANDS], high) + dot_t(bh[:BANDS], low) + dot_t(bl[:BANDS], high)) * (1.0 / CELLS)
        g = jnp.concatenate([g, jnp.zeros((BANDS, 96), F32)], axis=1)
        packed = g[0:4]
        for n in range(1, 4):
            packed = packed + pltpu.roll(g[4 * n : 4 * n + 4], 32 * n, 1)
        part[...] = packed
        col[p] = packed
        column_send(0, part, col)

    @pl.when(active)
    def _():
        total = column_sum(0, col)
        csum[...] = total
        full[my_slot] = total
        plane_send(0, csum, full, 17, slot_fft)

    def keep(a, h):
        hy[a] = h

    backward(keep)
    scatter(hy, 1)

    @pl.when(active)
    def _():
        total = plane_sum(0, full)

        @pl.when(p < 7)
        def _():
            g = jnp.concatenate([total] + [pltpu.roll(total, 128 - 32 * n, 1) for n in range(1, 4)], axis=0)
            u = inverse_rows(jnp.where(lane2 < 32, g, 0.0))
            w_high, w_low = split(jnp.where(lane2 < 16, u, -u)[:, :32])

            def rotated(high, low):
                return dot(w_high, high) + dot(w_high, low) + dot(w_low, high)

            q = rotated(bh[...], bl[...])
            for n in range(24):
                qs[pl.ds(n, BANDS, stride=24), :] = q[:, 128 * n : 128 * n + 128]

            def send(t, _):
                src = qs.at[pl.ds(pl.multiple_of(48 * t, 8), 48)]

                @pl.when(t == p)
                def _():
                    pltpu.make_async_copy(src, ob.at[p], r_o.at[p]).start()

                @pl.when(t != p)
                def _():
                    remote(src, ob.at[p], s_o.at[t], r_o.at[p], dev(t, i)).start()

                return 0

            lax.fori_loop(0, 8, send, 0)
            hq = rotated(*split(all_rows(1)))
            e = q[:, :128] * hq[:, :128]
            for n in range(1, 24):
                e = e + q[:, 128 * n : 128 * n + 128] * hq[:, 128 * n : 128 * n + 128]
            e = jnp.sum(e, axis=1, keepdims=True) * (1.0 / CELLS)
            row = lax.broadcasted_iota(jnp.int32, (16, 128), 0)
            e = jnp.sum(jnp.where(lane2 == row, e, 0.0), axis=0, keepdims=True)
            epart[...] = e
            ecol[p] = e
            column_send(1, epart, ecol)

        total = column_sum(1, ecol)
        ecsum[...] = total
        efull[my_slot] = total
        plane_send(1, ecsum, efull, 32, lambda n: n)

        for t in range(7):
            await_bytes(ob.at[t], r_o.at[t])
        zero = jnp.zeros((72, 128), F32)
        low_lanes, high_lanes = lane < 25, jnp.logical_and(lane >= 72, lane < 96)
        for k in range(6):
            j, jj = k // 3, k % 3
            rows = jnp.concatenate([ob[t, 8 * k : 8 * k + 8, :] for t in range(7)] + [zero], axis=0)
            if jj:
                rows = jnp.where(lone, 0.0, rows)
            rows = rows.T
            rows = jnp.where(low_lanes, rows, jnp.where(high_lanes, pltpu.roll(rows, 47, 1), 0.0))
            for c in range(2):
                grid[c, 0:25] = rows[64 * c : 64 * c + 25]
                grid[c, 25:72] = jnp.zeros((47, 128), F32)
                grid[c, 72:96] = rows[64 * c + 25 : 64 * c + BOX]
                o0, o1, o2, o3 = (grid[c, pl.ds(r, 24, stride=4), :] for r in range(4))
                thirds = (
                    jnp.where(lane < 96, o0, pltpu.roll(o1, 96, 1)),
                    jnp.where(lane < 64, pltpu.roll(o1, 96, 1), pltpu.roll(o2, 64, 1)),
                    jnp.where(lane < 32, pltpu.roll(o2, 64, 1), pltpu.roll(o3, 32, 1)),
                )
                for t in range(3):
                    xin[3 * c + jj, pl.ds(2 * t + j, 24, stride=6), :] = thirds[t]

    @pl.when(jnp.logical_not(active))
    def _():
        xin[...] = jnp.zeros((6, 144, 128), F32)

    pltpu.make_async_copy(xin, out_hbm, s_out.at[0]).start()
    e = plane_sum(1, efull)
    for j in range(2):
        energy_ref[j] = jnp.sum(jnp.where(lane == 2 * p + j, e, 0.0))
    weights = jax.nn.sigmoid((fermi_ref[0] - e) / TEMPER)
    band_energy_ref[0] = jnp.sum(jnp.where(lane < BANDS, weights * e, 0.0)) / float(BANDS)

    for k in range(6):
        valid, _, target = start_of(k)

        @pl.when(jnp.logical_and(valid, jnp.logical_not(is_me(target))))
        def _():
            await_bytes(xt.at[k], s_init.at[k])

    @pl.when(gives_v)
    def _():
        def one(g, _):
            @pl.when(jnp.logical_not(is_me(member_of(8 * y2 + g, i // 2))))
            def _():
                await_bytes(v_hbm, s_v.at[g])

            return 0

        lax.fori_loop(0, 8, one, 0)

    scattered(cur, 0)
    scattered(hy, 1)
    for w, (mine, mine2) in enumerate(((part, csum), (epart, ecsum))):

        @pl.when(summing)
        def _():
            def sent(t, _):
                @pl.when(t != p)
                def _():
                    await_bytes(mine, s_c.at[w, t])

                return 0

            lax.fori_loop(0, 8, sent, 0)

        @pl.when(active)
        def _():
            def sent(n, _):
                @pl.when((n if w else slot_fft(n)) != i)
                def _():
                    await_bytes(mine2, s_p.at[w, n])

                return 0

            lax.fori_loop(0, 32 if w else 17, sent, 0)

    @pl.when(summing)
    def _():
        def sent(t, _):
            @pl.when(t != p)
            def _():
                await_bytes(qs.at[pl.ds(pl.multiple_of(48 * t, 8), 48)], s_o.at[t])

            return 0

        lax.fori_loop(0, 8, sent, 0)

    await_bytes(xin, s_out.at[0])


def call(lower, upper, fermi, height, x, v):
    smem = pl.BlockSpec(memory_space=pltpu.SMEM)
    vmem = pl.BlockSpec(memory_space=pltpu.VMEM)
    hbm = pl.BlockSpec(memory_space=pl.ANY)
    sem = pltpu.SemaphoreType.DMA
    consts = tables()

    def buf(*shape):
        return pltpu.VMEM(shape, F32)

    return pl.pallas_call(
        kernel,
        out_shape=(
            jax.ShapeDtypeStruct((6, 144, 128), F32),
            jax.ShapeDtypeStruct((2,), F32),
            jax.ShapeDtypeStruct((1,), F32),
        ),
        in_specs=[smem] * 3 + [vmem] + [hbm] * 8,
        out_specs=(hbm, smem, smem),
        scratch_shapes=[
            buf(6, 144, 128),
            buf(2, 96, 128),
            *[pltpu.VMEM(t.shape, BF16) for t in consts],
            buf(6, 64, 128),
            buf(8, 64, 128),
            buf(6, 96, 96),
            buf(8, 64, 128),
            buf(8, 64, 128),
            buf(8, 64, 128),
            buf(8, 64, 128),
            buf(8, 64, 128),
            buf(2, 384, 128),
            buf(2, 7, 24, 128),
            buf(2, 7, 24, 128),
            buf(2, 384, 128),
            buf(2, 384, 128),
            pltpu.VMEM((32, 3072), BF16),
            pltpu.VMEM((32, 3072), BF16),
            buf(4, 128),
            buf(8, 4, 128),
            buf(4, 128),
            buf(17, 4, 128),
            buf(1, 128),
            buf(8, 1, 128),
            buf(1, 128),
            buf(17, 1, 128),
            buf(384, 128),
            buf(7, 48, 128),
            sem((1,)),
            sem((1,)),
            sem((6,)),
            sem((6,)),
            sem((8,)),
            sem((8,)),
            sem((2,)),
            sem((2, 16)),
            sem((2, 7)),
            sem((2, 7)),
            sem((2, 16)),
            sem((2, 56)),
            sem((2, 3, 16)),
            sem((2, 8)),
            sem((2, 8)),
            sem((2, 32)),
            sem((2, 17)),
            sem((8,)),
            sem((7,)),
            pltpu.SemaphoreType.REGULAR,
        ],
        compiler_params=pltpu.CompilerParams(
            has_side_effects=True, collective_id=0, vmem_limit_bytes=60 * 2**20
        ),
    )(lower, upper, fermi, height, x, v, *[jnp.asarray(t) for t in consts])


def local(start_bands, potential, half_height, lower_bound, upper_bound, fermi_level):
    x = start_bands.reshape(2, 2, 3, 72, 128).transpose(0, 2, 3, 1, 4).reshape(6, 144, 128)
    v = potential.transpose(2, 0, 1)
    out, energies, band_energy = call(lower_bound, upper_bound, fermi_level, half_height, x, v)
    out = out.reshape(2, 3, 72, 2, 128).transpose(0, 3, 1, 2, 4).reshape(2, 2, 3, NG * NG)
    return out, energies, band_energy


def solution(mesh):
    placed = (P(None, "band", "fft", None), P(None, None, "fft"), P("fft", None), P(), P(), P())
    return jax.shard_map(
        local,
        mesh=mesh,
        in_specs=placed,
        out_specs=(P(None, "band", "fft", None), P("band"), P()),
        check_vma=False,
    )
```

```python
import math

import jax
import jax.numpy as jnp
import ml_dtypes
import numpy as np
from jax import lax
from jax.experimental import pallas as pl
from jax.experimental.pallas import tpu as pltpu
from jax.sharding import PartitionSpec as P

NG = 96
CELLS = float(NG**3)
BOX = 49
KIN = 12.0 / 24**2
TEMPER = 0.5
BANDS = 16
ACTIVE = (*range(9), *range(24, 32))
MEMBERS = 16
HOLDERS = 7
ZP = 3
F32, BF16 = jnp.float32, jnp.bfloat16
MESH = pl.DeviceIdType.MESH


def box_frequency():
    r = np.arange(BOX)
    return np.where(r <= 24, r, r - BOX)


def halves(table):
    table = table.astype(np.float32)
    high = table.astype(ml_dtypes.bfloat16)
    low = (table - high.astype(np.float32)).astype(ml_dtypes.bfloat16)
    return high, low


def tables():
    freq = box_frequency()
    angle = 2.0 * math.pi / NG * ((np.arange(NG)[:, None] * freq[None, :]) % NG)
    cosine, sine = np.cos(angle), np.sin(angle)
    ahead = np.zeros((192, 64))
    ahead[:96, :BOX], ahead[96:, :BOX] = cosine, sine
    back = np.zeros((128, 96))
    back[:BOX], back[64 : 64 + BOX] = cosine.T, sine.T
    lanes = np.zeros((128, 256))
    lanes[:BOX, :96], lanes[:BOX, 128:224] = cosine.T, sine.T
    lanes[64 : 64 + BOX, :96], lanes[64 : 64 + BOX, 128:224] = -sine.T, cosine.T
    lanes_back = lanes.T.copy()
    plane = np.arange(NG).reshape(MEMBERS, 2, ZP)

    def left(t):
        high, low = halves(t)
        return np.concatenate([high, high, low], axis=1)

    def right(t):
        high, low = halves(t)
        return np.concatenate([high, high, low], axis=0)

    z_ahead = [np.concatenate([ahead[plane[:, h].ravel()], ahead[96 + plane[:, h].ravel()]]) for h in range(2)]
    z_back = [back[:, plane[:, h].ravel()] for h in range(2)]
    return (
        np.stack([left(t) for t in z_ahead]),
        left(ahead),
        np.stack([left(t) for t in z_back]),
        left(back),
        right(lanes),
        right(lanes_back),
    )


def split(x):
    high = x.astype(BF16)
    return high, (x - high.astype(F32)).astype(BF16)


def pieces(x, axis):
    high, low = split(x)
    return jnp.concatenate([high, low, high], axis=axis)


def dot(a, b):
    return jnp.dot(a, b, preferred_element_type=F32)


def dot_t(a, b):
    return lax.dot_general(a, b, (((1,), (1,)), ((), ())), preferred_element_type=F32)


def kernel(
    lower_ref,
    upper_ref,
    fermi_ref,
    height_hbm,
    x_hbm,
    v_hbm,
    tz_hbm,
    tx_hbm,
    tzb_hbm,
    txb_hbm,
    ty_hbm,
    tyb_hbm,
    out_hbm,
    energy_ref,
    band_energy_ref,
    xin,
    grid,
    height_ref,
    vin,
    vp,
    vb,
    vfull,
    acc,
    tz,
    tx,
    tzb,
    txb,
    ty,
    tyb,
    xt,
    x0,
    cur,
    prev,
    hy,
    inside,
    kin,
    sbuf,
    rbuf,
    bbuf,
    kbuf,
    gy,
    bh,
    bl,
    part,
    col,
    csum,
    full,
    epart,
    ecol,
    ecsum,
    efull,
    qs,
    ob,
    s_in,
    s_out,
    s_t,
    s_init,
    r_init,
    s_v,
    r_v,
    s_f,
    r_f,
    s_b,
    r_b,
    s_g,
    r_g,
    s_c,
    r_c,
    s_p,
    r_p,
    s_o,
    r_o,
    planes_in,
):
    p = lax.axis_index("band")
    i = lax.axis_index("fft")

    def quot(a, n):
        return a // n if isinstance(a, int) else lax.div(a, jnp.int32(n))

    def mod(a, n):
        return a % n if isinstance(a, int) else lax.rem(a, jnp.int32(n))

    def both(a, b):
        return jnp.logical_and(a, b)

    y, core = quot(p, 2), mod(p, 2)
    y2, yl = quot(y, 2), mod(y, 2)
    gx, gzz = quot(i, 8), mod(i, 8)
    x2, xl = quot(gx, 2), mod(gx, 2)
    gz, zl = quot(gzz, 2), mod(gzz, 2)
    band = 8 * y2 + 4 * x2 + gz
    xr = 2 * yl + mod(xl + yl, 2)
    zr = 2 * core + mod(zl + core, 2)
    place = 4 * xr + zr
    me = 4 * mod(xr + 2 * x2, 4) + mod(zr + gz, 4)
    chip = 2 * xr + zr - 2
    is_k = both(core == 1, chip < HOLDERS)
    active = jnp.logical_or(i <= 8, i >= 24)
    lone = i == 8
    summing = both(active, p < 7)

    def dev(pp, ii):
        return {"band": pp, "fft": ii}

    def at_place(yy, xx, zz, xr_, zr_):
        c = quot(zr_, 2)
        return dev(
            4 * yy + 2 * quot(xr_, 2) + c,
            16 * xx + 8 * mod(quot(xr_ + 1, 2), 2) + 2 * zz + mod(quot(zr_ + 1, 2), 2),
        )

    def holder(b, s):
        return at_place(quot(b, 8), mod(quot(b, 4), 2), mod(b, 4), quot(s, 2), 2 + mod(s, 2))

    def mine_at(n):
        return at_place(y2, x2, gz, n // 4, n % 4)

    def slab_of(n):
        return 4 * mod(n // 4 + 2 * x2, 4) + mod(n % 4 + gz, 4)

    def is_me(where):
        return both(where["band"] == p, where["fft"] == i)

    def remote(src, dst, ss, rs, where):
        return pltpu.make_async_remote_copy(
            src_ref=src, dst_ref=dst, send_sem=ss, recv_sem=rs, device_id=where, device_id_type=MESH
        )

    def await_bytes(ref, sem):
        pltpu.make_async_copy(ref, ref, sem).wait()

    for src, dst, n in ((x_hbm, xin, 0), (v_hbm, vin, 1), (height_hbm, height_ref, 2)):
        pltpu.make_async_copy(src, dst, s_in.at[n]).start()
    for n, (src, dst) in enumerate(
        ((tz_hbm, tz), (tx_hbm, tx), (tzb_hbm, tzb), (txb_hbm, txb), (ty_hbm, ty), (tyb_hbm, tyb))
    ):
        pltpu.make_async_copy(src, dst, s_t.at[n]).start()

    barrier = pltpu.get_barrier_semaphore()

    def tell(where):
        pl.semaphore_signal(barrier, inc=1, device_id=where, device_id_type=MESH)

    def kx_of_slot(a):
        q = 8 * chip + a
        return q < BOX, jnp.where(q <= 24, q, q + 47)

    @pl.when(is_k)
    def _():
        for a in range(8):
            held, kx = kx_of_slot(a)
            native = dev(quot(band, 2), quot(kx, 3))

            @pl.when(both(held, jnp.logical_not(is_me(native))))
            def _():
                tell(native)

    for h in range(2):
        source = dev(2 * y + quot(gz, 2), 2 * me + h)

        @pl.when(jnp.logical_not(is_me(source)))
        def _():
            tell(source)

    for n in range(MEMBERS):

        @pl.when(place != n)
        def _():
            tell(mine_at(n))

    def counterpart(n):
        return at_place(
            mod(y2 + n // 8, 2), mod(x2 + (n // 4) % 2, 2), mod(gz + n % 4, 4), xr, zr
        )

    for n in range(1, 16):
        tell(counterpart(n))

    def start_of(k):
        j, jj = k // 3, k % 3
        kx = 3 * i + jj
        valid = jnp.logical_or(kx <= 24, kx >= 72)
        q = jnp.where(kx <= 24, kx, kx - 47)
        s = jnp.minimum(jnp.maximum(quot(q, 8), 0), HOLDERS - 1)
        return valid, mod(q, 8), holder(2 * p + j, s)

    def v_target(n):
        xx = mod(quot(gx, 2) + yl, 2)
        zz = 2 * core + n
        return at_place(y2, xx, zz, mod(gx + 2 * xx, 4), mod(quot(gzz, 2) - zz + 4, 4))

    expected = jnp.int32(30)
    for k in range(6):
        valid, _, target = start_of(k)
        expected = expected + both(valid, jnp.logical_not(is_me(target))).astype(jnp.int32)
    for n in range(2):
        expected = expected + jnp.logical_not(is_me(v_target(n))).astype(jnp.int32)

    lane = lax.broadcasted_iota(jnp.int32, (1, 128), 1)
    sign = jnp.where(lane < 64, -1.0, 1.0).astype(F32)

    def swap(x):
        return pltpu.roll(x, 64, 1)

    def boxed_lanes(x):
        return jnp.where(lane < 25, x, jnp.where(lane < BOX, pltpu.roll(x, 128 - 47, 1), 0.0))

    def unpack(t0, t1, t2):
        return (
            t0,
            jnp.where(lane < 32, pltpu.roll(t0, 32, 1), pltpu.roll(t1, 32, 1)),
            jnp.where(lane < 64, pltpu.roll(t1, 64, 1), pltpu.roll(t2, 64, 1)),
            pltpu.roll(t2, 96, 1),
        )

    def pack(o0, o1, o2, o3):
        return (
            jnp.where(lane < 96, o0, pltpu.roll(o1, 96, 1)),
            jnp.where(lane < 64, pltpu.roll(o1, 96, 1), pltpu.roll(o2, 64, 1)),
            jnp.where(lane < 32, pltpu.roll(o2, 64, 1), pltpu.roll(o3, 32, 1)),
        )

    await_bytes(xin, s_in.at[0])
    await_bytes(height_ref, s_in.at[2])
    for k in range(6):
        j, jj = k // 3, k % 3
        for c in range(2):
            quarter = unpack(*(xin[3 * c + jj, pl.ds(2 * t + j, 24, stride=6), :] for t in range(3)))
            for r in range(4):
                grid[c, pl.ds(r, 24, stride=4), :] = boxed_lanes(quarter[r])
        pad = jnp.zeros((15, 128), F32)
        rows = jnp.concatenate([grid[0, 0:25], grid[0, 72:96], pad, grid[1, 0:25], grid[1, 72:96], pad], axis=0)
        xt[k] = rows.T[:56]
    for jj in range(3):
        h = height_ref[jj : jj + 1, :].astype(F32)
        h = boxed_lanes(jnp.concatenate([h, jnp.zeros((1, 32), F32)], axis=1))
        h = jnp.where(lane < BOX, h, -1.0)
        h = jnp.where(lane < 64, h, pltpu.roll(h, 64, 1))
        for j in range(2):
            xt[3 * j + jj, BOX : BOX + 1, :] = h
    await_bytes(vin, s_in.at[1])
    for z in range(3):
        grid[0] = jnp.concatenate([vin[z], jnp.zeros((96, 32), F32)], axis=1)
        thirds = pack(*(grid[0, pl.ds(r, 24, stride=4), :] for r in range(4)))
        for t in range(3):
            vp[z, 24 * t : 24 * t + 24, :] = thirds[t]

    pl.semaphore_wait(barrier, expected)

    for k in range(6):
        valid, slot, target = start_of(k)

        @pl.when(both(valid, is_me(target)))
        def _():
            pltpu.make_async_copy(xt.at[k], x0.at[slot], r_init.at[slot]).start()

        @pl.when(both(valid, jnp.logical_not(is_me(target))))
        def _():
            remote(xt.at[k], x0.at[slot], s_init.at[k], r_init.at[slot], target).start()

    for n in range(2):
        target = v_target(n)
        home = vb.at[pl.ds(3 * mod(i, 2), 3)]

        @pl.when(is_me(target))
        def _():
            pltpu.make_async_copy(vp, home, r_v.at[mod(i, 2)]).start()

        @pl.when(jnp.logical_not(is_me(target)))
        def _():
            remote(vp, home, s_v.at[n], r_v.at[mod(i, 2)], target).start()

    for n in range(1, 16):
        pl.semaphore_signal(planes_in, inc=1, device_id=counterpart(n), device_id_type=MESH)

    for n, dst in enumerate((tz, tx, tzb, txb, ty, tyb)):
        await_bytes(dst, s_t.at[n])

    @pl.when(is_k)
    def _():
        row = lax.broadcasted_iota(jnp.int32, (64, 128), 0)
        col_ = lax.broadcasted_iota(jnp.int32, (64, 128), 1) % 64
        fz = jnp.where(row <= 24, row, row - BOX)
        fy = jnp.where(col_ <= 24, col_, col_ - BOX)
        in_box = jnp.logical_and(row < BOX, col_ < BOX)
        yz = (fz * fz + fy * fy).astype(F32)
        absz = jnp.abs(fz).astype(F32)

        def plane(a, _):
            q = 8 * chip + a

            @pl.when(q < BOX)
            def _():
                await_bytes(x0.at[a], r_init.at[a])
                fx = jnp.where(q <= 24, q, q - BOX)
                data = x0[a]
                data = jnp.concatenate([data, jnp.zeros((8, 128), F32)], axis=0)
                keep = both(in_box, absz <= data[BOX : BOX + 1])
                cur[a] = jnp.where(keep, data, 0.0)
                inside[a] = jnp.where(keep, 1.0 / CELLS, 0.0)
                kin[a] = jnp.where(keep, KIN * (yz + (fx * fx).astype(F32)), 0.0)

            @pl.when(q >= BOX)
            def _():
                zero = jnp.zeros((64, 128), F32)
                cur[a] = zero
                inside[a] = zero
                kin[a] = zero

            prev[a] = jnp.zeros((64, 128), F32)
            return 0

        lax.fori_loop(0, 8, plane, 0)

    def message(m):
        return pl.ds(pl.multiple_of(24 * m, 8), 24)

    def forward():
        @pl.when(is_k)
        def _():
            x = pieces(jnp.concatenate([cur[a] for a in range(8)], axis=1), 0)
            for h in range(2):
                out = dot(tz[h], x)
                for a in range(8):
                    c, s = out[:48, 128 * a : 128 * a + 128], out[48:, 128 * a : 128 * a + 128]
                    sbuf[h, pl.ds(a, 48, stride=8), :] = c + sign * swap(s)

                for n in range(MEMBERS):
                    src = sbuf.at[h, message(slab_of(n))]
                    home = rbuf.at[h, chip]

                    @pl.when(place == n)
                    def _():
                        pltpu.make_async_copy(src, home, r_f.at[h]).start()

                    @pl.when(place != n)
                    def _():
                        remote(src, home, s_f.at[h], r_f.at[h], mine_at(n)).start()

    def middle(first):
        zero8 = jnp.zeros((8, 128), F32)
        for h in range(2):
            await_bytes(rbuf.at[h], r_f.at[h])
            d = jnp.concatenate(
                [
                    jnp.concatenate(
                        [rbuf[h, s, 8 * z : 8 * z + 8, :] for s in range(HOLDERS)] + [zero8], axis=0
                    )
                    for z in range(ZP)
                ],
                axis=1,
            )
            out = dot(tx[...], pieces(d, 0))
            rows = jnp.concatenate(
                [
                    out[:96, 128 * z : 128 * z + 128] + sign * swap(out[96:, 128 * z : 128 * z + 128])
                    for z in range(ZP)
                ],
                axis=0,
            )
            psi = dot(pieces(rows, 1), ty[...])

            @pl.when(first)
            def _():
                await_bytes(vb.at[pl.ds(3 * h, 3)], r_v.at[h])
                for z in range(3 * h, 3 * h + 3):
                    quarter = unpack(*(vb[z, 24 * t : 24 * t + 24, :] for t in range(3)))
                    for r in range(4):
                        vfull[z, pl.ds(r, 24, stride=4), :] = jnp.where(lane < NG, quarter[r], 0.0)

            v = jnp.concatenate([vfull[3 * h + z] for z in range(ZP)], axis=0)
            psi = psi * jnp.concatenate([v, v], axis=1)
            rows = dot(pieces(psi, 1), tyb[...])
            d = jnp.concatenate([rows[96 * z : 96 * z + 96] for z in range(ZP)], axis=1)
            out = dot(txb[...], pieces(d, 0))
            for z in range(ZP):
                o = out[:64, 128 * z : 128 * z + 128] - sign * swap(out[64:, 128 * z : 128 * z + 128])
                for s in range(HOLDERS):
                    bbuf[h, s, 8 * z : 8 * z + 8, :] = o[8 * s : 8 * s + 8]

            for s in range(HOLDERS):
                home = kbuf.at[h, message(me)]
                mine = both(is_k, chip == s)

                @pl.when(mine)
                def _():
                    pltpu.make_async_copy(bbuf.at[h, s], home, r_b.at[h]).start()

                @pl.when(jnp.logical_not(mine))
                def _():
                    remote(bbuf.at[h, s], home, s_b.at[h], r_b.at[h], mine_at(4 * (s // 2) + 2 + s % 2)).start()

    def backward(finish):
        @pl.when(is_k)
        def _():
            for h in range(2):
                await_bytes(kbuf.at[h], r_b.at[h])
                d = jnp.concatenate([kbuf[h, pl.ds(a, 48, stride=8), :] for a in range(8)], axis=1)
                term = dot(tzb[h], pieces(d, 0))
                acc[...] = acc[...] + term if h else term
            for a in range(8):
                f = acc[:64, 128 * a : 128 * a + 128] - sign * swap(acc[64:, 128 * a : 128 * a + 128])
                finish(a, kin[a] * cur[a] + inside[a] * f)
            for h in range(2):
                await_bytes(sbuf.at[h, pl.ds(0, 24 * (MEMBERS - 1))], s_f.at[h])
                await_bytes(bbuf.at[h, pl.ds(0, HOLDERS - 1)], s_b.at[h])

        @pl.when(jnp.logical_not(is_k))
        def _():
            for h in range(2):
                await_bytes(bbuf.at[h], s_b.at[h])

    center = 0.5 * (upper_ref[0] + lower_ref[0])
    half_width = 0.5 * (upper_ref[0] - lower_ref[0])

    def step(k, _):
        forward()
        middle(k == 0)
        alpha = jnp.where(k == 0, 1.0, 2.0).astype(F32)
        beta = jnp.where(k == 0, 0.0, 1.0).astype(F32)

        def finish(a, h):
            old = cur[a]
            new = alpha * (h - center * old) / half_width - beta * prev[a]
            prev[a] = old
            cur[a] = new

        backward(finish)
        return 0

    lax.fori_loop(0, 3, step, 0)

    def for_rows(do):
        @pl.when(is_k)
        def _():
            for a in range(8):
                held, kx = kx_of_slot(a)
                home, jj = quot(kx, 3), mod(kx, 3)

                @pl.when(held)
                def _():
                    for t in range(7):
                        target = dev(t, home)
                        do(a, t, jj, target)

    def scatter(src, w):
        def one(a, t, jj, target):
            dst = gy.at[w, pl.ds(pl.multiple_of(128 * jj + 8 * band, 8), 8)]
            row = src.at[a, pl.ds(8 * t, 8)]

            @pl.when(is_me(target))
            def _():
                pltpu.make_async_copy(row, dst, r_g.at[w]).start()

            @pl.when(jnp.logical_not(is_me(target)))
            def _():
                remote(row, dst, s_g.at[w, 7 * a + t], r_g.at[w], target).start()

        for_rows(one)

    def scattered(src, w):
        def one(a, t, jj, target):
            @pl.when(jnp.logical_not(is_me(target)))
            def _():
                await_bytes(src.at[a, pl.ds(8 * t, 8)], s_g.at[w, 7 * a + t])

        for_rows(one)

    def all_rows(w):
        @pl.when(lone)
        def _():
            await_bytes(gy.at[w, pl.ds(0, 128)], r_g.at[w])

        @pl.when(jnp.logical_not(lone))
        def _():
            await_bytes(gy.at[w], r_g.at[w])

        rows = []
        for jj in range(3):
            for r in range(8):
                x = gy[w, pl.ds(128 * jj + r, BANDS, stride=8), :]
                rows.append(jnp.where(lone, 0.0, x) if jj else x)
        a = jnp.concatenate(rows, axis=1)
        b = jnp.concatenate([-sign * swap(x) for x in rows], axis=1)
        return jnp.concatenate([a, b], axis=0)

    my_slot = jnp.minimum(jnp.where(i <= 8, i, jnp.maximum(i - 15, 0)), 16)

    def column_send(w, mine, theirs):
        for t in range(8):

            @pl.when(p != t)
            def _():
                remote(mine, theirs.at[p], s_c.at[w], r_c.at[w], dev(t, i)).start()

    def column_sum(w, theirs):
        @pl.when(p < 7)
        def _():
            await_bytes(theirs.at[pl.ds(0, 6)], r_c.at[w])

        @pl.when(p == 7)
        def _():
            await_bytes(theirs.at[pl.ds(0, 7)], r_c.at[w])

        total = theirs[0]
        for t in range(1, 7):
            total = total + theirs[t]
        return total

    def plane_send(w, mine, theirs, targets):
        for ii in targets:

            @pl.when(i != ii)
            def _():
                remote(mine, theirs.at[my_slot], s_p.at[w], r_p.at[w], dev(p, ii)).start()

    def plane_sum(w, theirs):
        @pl.when(active)
        def _():
            await_bytes(theirs.at[pl.ds(0, 16)], r_p.at[w])

        @pl.when(jnp.logical_not(active))
        def _():
            await_bytes(theirs.at[pl.ds(0, 17)], r_p.at[w])

        total = theirs[0]
        for n in range(1, 17):
            total = total + theirs[n]
        return total

    lane2 = lax.broadcasted_iota(jnp.int32, (16, 128), 1)

    def inverse_rows(g):
        row = lax.broadcasted_iota(jnp.int32, (32, 128), 0)
        ln = lax.broadcasted_iota(jnp.int32, (32, 128), 1)
        top = jnp.where(lane2 < 16, g, -g)
        bottom = jnp.where(lane2 < 16, pltpu.roll(g, 112, 1), pltpu.roll(g, 16, 1))
        m = jnp.where(ln < 32, jnp.concatenate([top, bottom], 0), 0.0)
        m = m + jnp.where(ln == row + 32, 1.0, 0.0)
        for j in range(32):
            pivot = m[j : j + 1, :]
            factor = m[:, j : j + 1] * (1.0 / pivot[:, j : j + 1])
            m = m - jnp.where(row > j, factor, 0.0) * pivot
        diag = jnp.sum(jnp.where(ln == row, m, 0.0), axis=1, keepdims=True)
        u = m[:16] / jnp.sqrt(diag[:16])
        return jnp.where(lane2 < 32, pltpu.roll(u, 96, 1), 0.0)

    pl.semaphore_wait(planes_in, 15)
    scatter(cur, 0)
    forward()
    middle(False)

    @pl.when(summing)
    def _():
        high, low = split(all_rows(0))
        bh[...] = high
        bl[...] = low
        g = (dot_t(bh[:BANDS], high) + dot_t(bh[:BANDS], low) + dot_t(bl[:BANDS], high)) * (1.0 / CELLS)
        g = jnp.concatenate([g, jnp.zeros((BANDS, 96), F32)], axis=1)
        packed = g[0:4]
        for n in range(1, 4):
            packed = packed + pltpu.roll(g[4 * n : 4 * n + 4], 32 * n, 1)
        part[...] = packed
        col[p] = packed
        column_send(0, part, col)

    @pl.when(active)
    def _():
        total = column_sum(0, col)
        csum[...] = total
        full[my_slot] = total
        plane_send(0, csum, full, ACTIVE)

    def keep(a, h):
        hy[a] = h

    backward(keep)
    scatter(hy, 1)

    @pl.when(active)
    def _():
        total = plane_sum(0, full)

        @pl.when(p < 7)
        def _():
            g = jnp.concatenate([total] + [pltpu.roll(total, 128 - 32 * n, 1) for n in range(1, 4)], axis=0)
            u = inverse_rows(jnp.where(lane2 < 32, g, 0.0))
            w_high, w_low = split(jnp.where(lane2 < 16, u, -u)[:, :32])

            def rotated(high, low):
                return dot(w_high, high) + dot(w_high, low) + dot(w_low, high)

            q = rotated(bh[...], bl[...])
            for n in range(24):
                qs[pl.ds(n, BANDS, stride=24), :] = q[:, 128 * n : 128 * n + 128]

            for t in range(8):
                src = qs.at[pl.ds(48 * t, 48)]

                @pl.when(p == t)
                def _():
                    pltpu.make_async_copy(src, ob.at[p], r_o.at[0]).start()

                @pl.when(p != t)
                def _():
                    remote(src, ob.at[p], s_o.at[0], r_o.at[0], dev(t, i)).start()

            hq = rotated(*split(all_rows(1)))
            e = q[:, :128] * hq[:, :128]
            for n in range(1, 24):
                e = e + q[:, 128 * n : 128 * n + 128] * hq[:, 128 * n : 128 * n + 128]
            e = jnp.sum(e, axis=1, keepdims=True) * (1.0 / CELLS)
            row = lax.broadcasted_iota(jnp.int32, (16, 128), 0)
            e = jnp.sum(jnp.where(lane2 == row, e, 0.0), axis=0, keepdims=True)
            epart[...] = e
            ecol[p] = e
            column_send(1, epart, ecol)

        total = column_sum(1, ecol)
        ecsum[...] = total
        efull[my_slot] = total
        plane_send(1, ecsum, efull, range(32))

        await_bytes(ob, r_o.at[0])
        zero = jnp.zeros((72, 128), F32)
        low_lanes, high_lanes = lane < 25, jnp.logical_and(lane >= 72, lane < 96)
        for k in range(6):
            j, jj = k // 3, k % 3
            rows = jnp.concatenate([ob[t, 8 * k : 8 * k + 8, :] for t in range(7)] + [zero], axis=0)
            if jj:
                rows = jnp.where(lone, 0.0, rows)
            rows = rows.T
            rows = jnp.where(low_lanes, rows, jnp.where(high_lanes, pltpu.roll(rows, 47, 1), 0.0))
            for c in range(2):
                grid[c, 0:25] = rows[64 * c : 64 * c + 25]
                grid[c, 25:72] = jnp.zeros((47, 128), F32)
                grid[c, 72:96] = rows[64 * c + 25 : 64 * c + BOX]
                thirds = pack(*(grid[c, pl.ds(r, 24, stride=4), :] for r in range(4)))
                for t in range(3):
                    xin[3 * c + jj, pl.ds(2 * t + j, 24, stride=6), :] = thirds[t]

    @pl.when(jnp.logical_not(active))
    def _():
        xin[...] = jnp.zeros((6, 144, 128), F32)

    pltpu.make_async_copy(xin, out_hbm, s_out.at[0]).start()

    for k in range(6):
        valid, _, target = start_of(k)

        @pl.when(both(valid, jnp.logical_not(is_me(target))))
        def _():
            await_bytes(xt.at[k], s_init.at[k])

    for n in range(2):

        @pl.when(jnp.logical_not(is_me(v_target(n))))
        def _():
            await_bytes(vp, s_v.at[n])

    scattered(cur, 0)
    scattered(hy, 1)

    @pl.when(summing)
    def _():
        await_bytes(col.at[pl.ds(0, 7)], s_c.at[0])
        await_bytes(ecol.at[pl.ds(0, 7)], s_c.at[1])
        await_bytes(qs.at[pl.ds(0, 48 * 7)], s_o.at[0])

    @pl.when(active)
    def _():
        await_bytes(full.at[pl.ds(0, 16)], s_p.at[0])
        await_bytes(efull.at[pl.ds(0, 31)], s_p.at[1])

    await_bytes(xin, s_out.at[0])

    e = plane_sum(1, efull)
    for j in range(2):
        energy_ref[j] = jnp.sum(jnp.where(lane == 2 * p + j, e, 0.0))
    weights = jax.nn.sigmoid((fermi_ref[0] - e) / TEMPER)
    band_energy_ref[0] = jnp.sum(jnp.where(lane < BANDS, weights * e, 0.0)) / float(BANDS)


def call(lower, upper, fermi, height, x, v):
    smem = pl.BlockSpec(memory_space=pltpu.SMEM)
    hbm = pl.BlockSpec(memory_space=pl.ANY)
    sem = pltpu.SemaphoreType.DMA
    consts = tables()

    def buf(*shape):
        return pltpu.VMEM(shape, F32)

    return pl.pallas_call(
        kernel,
        out_shape=(
            jax.ShapeDtypeStruct((6, 144, 128), F32),
            jax.ShapeDtypeStruct((2,), F32),
            jax.ShapeDtypeStruct((1,), F32),
        ),
        in_specs=[smem] * 3 + [hbm] * 9,
        out_specs=(hbm, smem, smem),
        scratch_shapes=[
            buf(6, 144, 128),
            buf(2, 96, 128),
            pltpu.VMEM((3, 96), jnp.int32),
            buf(3, 96, 96),
            buf(3, 72, 128),
            buf(6, 72, 128),
            buf(6, 96, 128),
            buf(128, 1024),
            *[pltpu.VMEM(t.shape, BF16) for t in consts],
            buf(6, 56, 128),
            buf(8, 56, 128),
            buf(8, 64, 128),
            buf(8, 64, 128),
            buf(8, 64, 128),
            buf(8, 64, 128),
            buf(8, 64, 128),
            buf(2, 384, 128),
            buf(2, 7, 24, 128),
            buf(2, 7, 24, 128),
            buf(2, 384, 128),
            buf(2, 384, 128),
            pltpu.VMEM((32, 3072), BF16),
            pltpu.VMEM((32, 3072), BF16),
            buf(4, 128),
            buf(8, 4, 128),
            buf(4, 128),
            buf(17, 4, 128),
            buf(1, 128),
            buf(8, 1, 128),
            buf(1, 128),
            buf(32, 1, 128),
            buf(384, 128),
            buf(7, 48, 128),
            sem((3,)),
            sem((1,)),
            sem((6,)),
            sem((6,)),
            sem((8,)),
            sem((2,)),
            sem((2,)),
            sem((2,)),
            sem((2,)),
            sem((2,)),
            sem((2,)),
            sem((2, 56)),
            sem((2,)),
            sem((2,)),
            sem((2,)),
            sem((2,)),
            sem((2,)),
            sem((1,)),
            sem((1,)),
            pltpu.SemaphoreType.REGULAR,
        ],
        compiler_params=pltpu.CompilerParams(
            has_side_effects=True, collective_id=0, vmem_limit_bytes=60 * 2**20
        ),
    )(lower, upper, fermi, height, x, v, *[jnp.asarray(t) for t in consts])


def local(start_bands, potential, half_height, lower_bound, upper_bound, fermi_level):
    x = start_bands.reshape(2, 2, 3, 72, 128).transpose(0, 2, 3, 1, 4).reshape(6, 144, 128)
    v = potential.transpose(2, 0, 1)
    out, energies, band_energy = call(lower_bound, upper_bound, fermi_level, half_height, x, v)
    out = out.reshape(2, 3, 72, 2, 128).transpose(0, 3, 1, 2, 4).reshape(2, 2, 3, NG * NG)
    return out, energies, band_energy


def solution(mesh):
    placed = (P(None, "band", "fft", None), P(None, None, "fft"), P("fft", None), P(), P(), P())
    return jax.shard_map(
        local,
        mesh=mesh,
        in_specs=placed,
        out_specs=(P(None, "band", "fft", None), P("band"), P()),
        check_vma=False,
    )
```

```python
import math

import jax
import jax.numpy as jnp
import ml_dtypes
import numpy as np
from jax import lax
from jax.experimental import pallas as pl
from jax.experimental.pallas import tpu as pltpu
from jax.sharding import PartitionSpec as P

NG = 96
CELLS = float(NG**3)
BOX = 49
KIN = 12.0 / 24**2
TEMPER = 0.5
BANDS = 16
ACTIVE = (*range(9), *range(24, 32))
MEMBERS = 16
HOLDERS = 7
ZP = 3
F32, BF16 = jnp.float32, jnp.bfloat16
MESH = pl.DeviceIdType.MESH


def box_frequency():
    r = np.arange(BOX)
    return np.where(r <= 24, r, r - BOX)


def halves(table):
    table = table.astype(np.float32)
    high = table.astype(ml_dtypes.bfloat16)
    low = (table - high.astype(np.float32)).astype(ml_dtypes.bfloat16)
    return high, low


def tables():
    freq = box_frequency()
    angle = 2.0 * math.pi / NG * ((np.arange(NG)[:, None] * freq[None, :]) % NG)
    cosine, sine = np.cos(angle), np.sin(angle)
    ahead = np.zeros((192, 64))
    ahead[:96, :BOX], ahead[96:, :BOX] = cosine, sine
    back = np.zeros((128, 96))
    back[:BOX], back[64 : 64 + BOX] = cosine.T, sine.T
    lanes = np.zeros((128, 256))
    lanes[:BOX, :96], lanes[:BOX, 128:224] = cosine.T, sine.T
    lanes[64 : 64 + BOX, :96], lanes[64 : 64 + BOX, 128:224] = -sine.T, cosine.T
    lanes_back = lanes.T.copy()
    plane = np.arange(NG).reshape(MEMBERS, 2, ZP)

    def left(t):
        high, low = halves(t)
        return np.concatenate([high, high, low], axis=1)

    def right(t):
        high, low = halves(t)
        return np.concatenate([high, high, low], axis=0)

    z_ahead = [np.concatenate([ahead[plane[:, h].ravel()], ahead[96 + plane[:, h].ravel()]]) for h in range(2)]
    z_back = [back[:, plane[:, h].ravel()] for h in range(2)]
    return (
        np.stack([left(t) for t in z_ahead]),
        left(ahead),
        np.stack([left(t) for t in z_back]),
        left(back),
        right(lanes),
        right(lanes_back),
    )


def split(x):
    high = x.astype(BF16)
    return high, (x - high.astype(F32)).astype(BF16)


def pieces(x, axis):
    high, low = split(x)
    return jnp.concatenate([high, low, high], axis=axis)


def dot(a, b):
    return jnp.dot(a, b, preferred_element_type=F32)


def dot_t(a, b):
    return lax.dot_general(a, b, (((1,), (1,)), ((), ())), preferred_element_type=F32)


def kernel(
    lower_ref,
    upper_ref,
    fermi_ref,
    height_hbm,
    x_hbm,
    v_hbm,
    tz_hbm,
    tx_hbm,
    tzb_hbm,
    txb_hbm,
    ty_hbm,
    tyb_hbm,
    out_hbm,
    energy_ref,
    band_energy_ref,
    xin,
    grid,
    height_ref,
    vin,
    vp,
    vb,
    vfull,
    acc,
    tz,
    tx,
    tzb,
    txb,
    ty,
    tyb,
    xt,
    x0,
    cur,
    prev,
    hy,
    inside,
    kin,
    sbuf,
    rbuf,
    bbuf,
    kbuf,
    gy,
    bh,
    bl,
    part,
    full,
    epart,
    efull,
    qs,
    ob,
    s_in,
    s_out,
    s_t,
    s_init,
    r_init,
    s_v,
    r_v,
    s_f,
    r_f,
    s_b,
    r_b,
    s_g,
    r_g,
    s_p,
    r_p,
    s_o,
    r_o,
    planes_in,
):
    p = lax.axis_index("band")
    i = lax.axis_index("fft")

    def quot(a, n):
        return a // n if isinstance(a, int) else lax.div(a, jnp.int32(n))

    def mod(a, n):
        return a % n if isinstance(a, int) else lax.rem(a, jnp.int32(n))

    def both(a, b):
        return jnp.logical_and(a, b)

    y, core = quot(p, 2), mod(p, 2)
    y2, yl = quot(y, 2), mod(y, 2)
    gx, gzz = quot(i, 8), mod(i, 8)
    x2, xl = quot(gx, 2), mod(gx, 2)
    gz, zl = quot(gzz, 2), mod(gzz, 2)
    band = 8 * y2 + 4 * x2 + gz
    xr = 2 * yl + mod(xl + yl, 2)
    zr = 2 * core + mod(zl + core, 2)
    place = 4 * xr + zr
    me = 4 * mod(xr + 2 * x2, 4) + mod(zr + 2 * quot(gz, 2), 4)
    chip = 2 * xr + zr - 2
    is_k = both(core == 1, chip < HOLDERS)
    active = jnp.logical_or(i <= 8, i >= 24)
    lone = i == 8

    def dev(pp, ii):
        return {"band": pp, "fft": ii}

    def at_place(yy, xx, zz, xr_, zr_):
        c = quot(zr_, 2)
        return dev(
            4 * yy + 2 * quot(xr_, 2) + c,
            16 * xx + 8 * mod(quot(xr_ + 1, 2), 2) + 2 * zz + mod(quot(zr_ + 1, 2), 2),
        )

    def holder(b, s):
        return at_place(quot(b, 8), mod(quot(b, 4), 2), mod(b, 4), quot(s, 2), 2 + mod(s, 2))

    def mine_at(n):
        return at_place(y2, x2, gz, n // 4, n % 4)

    def slab_of(n):
        return 4 * mod(n // 4 + 2 * x2, 4) + mod(n % 4 + 2 * quot(gz, 2), 4)

    def is_me(where):
        return both(where["band"] == p, where["fft"] == i)

    def remote(src, dst, ss, rs, where):
        return pltpu.make_async_remote_copy(
            src_ref=src, dst_ref=dst, send_sem=ss, recv_sem=rs, device_id=where, device_id_type=MESH
        )

    def await_bytes(ref, sem):
        pltpu.make_async_copy(ref, ref, sem).wait()

    for src, dst, n in ((x_hbm, xin, 0), (v_hbm, vin, 1), (height_hbm, height_ref, 2)):
        pltpu.make_async_copy(src, dst, s_in.at[n]).start()
    for n, (src, dst) in enumerate(
        ((tz_hbm, tz), (tx_hbm, tx), (tzb_hbm, tzb), (txb_hbm, txb), (ty_hbm, ty), (tyb_hbm, tyb))
    ):
        pltpu.make_async_copy(src, dst, s_t.at[n]).start()

    barrier = pltpu.get_barrier_semaphore()

    def tell(where):
        pl.semaphore_signal(barrier, inc=1, device_id=where, device_id_type=MESH)

    def kx_of_slot(a):
        q = 8 * chip + a
        return q < BOX, jnp.where(q <= 24, q, q + 47)

    @pl.when(is_k)
    def _():
        for a in range(8):
            held, kx = kx_of_slot(a)
            native = dev(quot(band, 2), quot(kx, 3))

            @pl.when(both(held, jnp.logical_not(is_me(native))))
            def _():
                tell(native)

    for h in range(2):
        source = dev(2 * y + quot(gz, 2), 2 * me + h)

        @pl.when(jnp.logical_not(is_me(source)))
        def _():
            tell(source)

    for n in range(MEMBERS):

        @pl.when(place != n)
        def _():
            tell(mine_at(n))

    def counterpart(n):
        return at_place(
            mod(y2 + n // 8, 2), mod(x2 + (n // 4) % 2, 2), mod(gz + n % 4, 4), xr, zr
        )

    for n in range(1, 16):
        tell(counterpart(n))

    def start_of(k):
        j, jj = k // 3, k % 3
        kx = 3 * i + jj
        valid = jnp.logical_or(kx <= 24, kx >= 72)
        q = jnp.where(kx <= 24, kx, kx - 47)
        s = jnp.minimum(jnp.maximum(quot(q, 8), 0), HOLDERS - 1)
        return valid, mod(q, 8), holder(2 * p + j, s)

    def v_target(n):
        xx = mod(quot(gx, 2) + yl, 2)
        return at_place(y2, xx, 2 * core + n, mod(gx + 2 * xx, 4), mod(quot(gzz, 2) + 2 * core, 4))

    expected = jnp.int32(30)
    for k in range(6):
        valid, _, target = start_of(k)
        expected = expected + both(valid, jnp.logical_not(is_me(target))).astype(jnp.int32)
    for n in range(2):
        expected = expected + jnp.logical_not(is_me(v_target(n))).astype(jnp.int32)

    lane = lax.broadcasted_iota(jnp.int32, (1, 128), 1)
    sign = jnp.where(lane < 64, -1.0, 1.0).astype(F32)

    def swap(x):
        return pltpu.roll(x, 64, 1)

    def boxed_lanes(x):
        return jnp.where(lane < 25, x, jnp.where(lane < BOX, pltpu.roll(x, 128 - 47, 1), 0.0))

    def unpack(t0, t1, t2):
        return (
            t0,
            jnp.where(lane < 32, pltpu.roll(t0, 32, 1), pltpu.roll(t1, 32, 1)),
            jnp.where(lane < 64, pltpu.roll(t1, 64, 1), pltpu.roll(t2, 64, 1)),
            pltpu.roll(t2, 96, 1),
        )

    def pack(o0, o1, o2, o3):
        return (
            jnp.where(lane < 96, o0, pltpu.roll(o1, 96, 1)),
            jnp.where(lane < 64, pltpu.roll(o1, 96, 1), pltpu.roll(o2, 64, 1)),
            jnp.where(lane < 32, pltpu.roll(o2, 64, 1), pltpu.roll(o3, 32, 1)),
        )

    await_bytes(xin, s_in.at[0])
    await_bytes(height_ref, s_in.at[2])
    for k in range(6):
        j, jj = k // 3, k % 3
        for c in range(2):
            quarter = unpack(*(xin[3 * c + jj, pl.ds(2 * t + j, 24, stride=6), :] for t in range(3)))
            for r in range(4):
                grid[c, pl.ds(r, 24, stride=4), :] = boxed_lanes(quarter[r])
        pad = jnp.zeros((15, 128), F32)
        rows = jnp.concatenate([grid[0, 0:25], grid[0, 72:96], pad, grid[1, 0:25], grid[1, 72:96], pad], axis=0)
        xt[k] = rows.T[:56]
    for jj in range(3):
        h = height_ref[jj : jj + 1, :].astype(F32)
        h = boxed_lanes(jnp.concatenate([h, jnp.zeros((1, 32), F32)], axis=1))
        h = jnp.where(lane < BOX, h, -1.0)
        h = jnp.where(lane < 64, h, pltpu.roll(h, 64, 1))
        for j in range(2):
            xt[3 * j + jj, BOX : BOX + 1, :] = h
    await_bytes(vin, s_in.at[1])
    for z in range(3):
        grid[0] = jnp.concatenate([vin[z], jnp.zeros((96, 32), F32)], axis=1)
        thirds = pack(*(grid[0, pl.ds(r, 24, stride=4), :] for r in range(4)))
        for t in range(3):
            vp[z, 24 * t : 24 * t + 24, :] = thirds[t]

    pl.semaphore_wait(barrier, expected)

    for k in range(6):
        valid, slot, target = start_of(k)

        @pl.when(both(valid, is_me(target)))
        def _():
            pltpu.make_async_copy(xt.at[k], x0.at[slot], r_init.at[slot]).start()

        @pl.when(both(valid, jnp.logical_not(is_me(target))))
        def _():
            remote(xt.at[k], x0.at[slot], s_init.at[k], r_init.at[slot], target).start()

    for n in range(2):
        target = v_target(n)
        home = vb.at[pl.ds(3 * mod(i, 2), 3)]

        @pl.when(is_me(target))
        def _():
            pltpu.make_async_copy(vp, home, r_v.at[mod(i, 2)]).start()

        @pl.when(jnp.logical_not(is_me(target)))
        def _():
            remote(vp, home, s_v.at[n], r_v.at[mod(i, 2)], target).start()

    for n in range(1, 16):
        pl.semaphore_signal(planes_in, inc=1, device_id=counterpart(n), device_id_type=MESH)

    for n, dst in enumerate((tz, tx, tzb, txb, ty, tyb)):
        await_bytes(dst, s_t.at[n])

    @pl.when(is_k)
    def _():
        row = lax.broadcasted_iota(jnp.int32, (64, 128), 0)
        col_ = lax.broadcasted_iota(jnp.int32, (64, 128), 1) % 64
        fz = jnp.where(row <= 24, row, row - BOX)
        fy = jnp.where(col_ <= 24, col_, col_ - BOX)
        in_box = jnp.logical_and(row < BOX, col_ < BOX)
        yz = (fz * fz + fy * fy).astype(F32)
        absz = jnp.abs(fz).astype(F32)

        def plane(a, _):
            q = 8 * chip + a

            @pl.when(q < BOX)
            def _():
                await_bytes(x0.at[a], r_init.at[a])
                fx = jnp.where(q <= 24, q, q - BOX)
                data = x0[a]
                data = jnp.concatenate([data, jnp.zeros((8, 128), F32)], axis=0)
                keep = both(in_box, absz <= data[BOX : BOX + 1])
                cur[a] = jnp.where(keep, data, 0.0)
                inside[a] = jnp.where(keep, 1.0 / CELLS, 0.0)
                kin[a] = jnp.where(keep, KIN * (yz + (fx * fx).astype(F32)), 0.0)

            @pl.when(q >= BOX)
            def _():
                zero = jnp.zeros((64, 128), F32)
                cur[a] = zero
                inside[a] = zero
                kin[a] = zero

            prev[a] = jnp.zeros((64, 128), F32)
            return 0

        lax.fori_loop(0, 8, plane, 0)

    def message(m):
        return pl.ds(pl.multiple_of(24 * m, 8), 24)

    def forward():
        @pl.when(is_k)
        def _():
            x = pieces(jnp.concatenate([cur[a] for a in range(8)], axis=1), 0)
            for h in range(2):
                out = dot(tz[h], x)
                for a in range(8):
                    c, s = out[:48, 128 * a : 128 * a + 128], out[48:, 128 * a : 128 * a + 128]
                    sbuf[h, pl.ds(a, 48, stride=8), :] = c + sign * swap(s)

                for n in range(MEMBERS):
                    src = sbuf.at[h, message(slab_of(n))]
                    home = rbuf.at[h, chip]

                    @pl.when(place == n)
                    def _():
                        pltpu.make_async_copy(src, home, r_f.at[h]).start()

                    @pl.when(place != n)
                    def _():
                        remote(src, home, s_f.at[h], r_f.at[h], mine_at(n)).start()

    def middle(first):
        zero8 = jnp.zeros((8, 128), F32)
        for h in range(2):
            await_bytes(rbuf.at[h], r_f.at[h])
            d = jnp.concatenate(
                [
                    jnp.concatenate(
                        [rbuf[h, s, 8 * z : 8 * z + 8, :] for s in range(HOLDERS)] + [zero8], axis=0
                    )
                    for z in range(ZP)
                ],
                axis=1,
            )
            out = dot(tx[...], pieces(d, 0))
            rows = jnp.concatenate(
                [
                    out[:96, 128 * z : 128 * z + 128] + sign * swap(out[96:, 128 * z : 128 * z + 128])
                    for z in range(ZP)
                ],
                axis=0,
            )
            psi = dot(pieces(rows, 1), ty[...])

            @pl.when(first)
            def _():
                await_bytes(vb.at[pl.ds(3 * h, 3)], r_v.at[h])
                for z in range(3 * h, 3 * h + 3):
                    quarter = unpack(*(vb[z, 24 * t : 24 * t + 24, :] for t in range(3)))
                    for r in range(4):
                        vfull[z, pl.ds(r, 24, stride=4), :] = jnp.where(lane < NG, quarter[r], 0.0)

            v = jnp.concatenate([vfull[3 * h + z] for z in range(ZP)], axis=0)
            psi = psi * jnp.concatenate([v, v], axis=1)
            rows = dot(pieces(psi, 1), tyb[...])
            d = jnp.concatenate([rows[96 * z : 96 * z + 96] for z in range(ZP)], axis=1)
            out = dot(txb[...], pieces(d, 0))
            for z in range(ZP):
                o = out[:64, 128 * z : 128 * z + 128] - sign * swap(out[64:, 128 * z : 128 * z + 128])
                for s in range(HOLDERS):
                    bbuf[h, s, 8 * z : 8 * z + 8, :] = o[8 * s : 8 * s + 8]

            for s in range(HOLDERS):
                home = kbuf.at[h, message(me)]
                mine = both(is_k, chip == s)

                @pl.when(mine)
                def _():
                    pltpu.make_async_copy(bbuf.at[h, s], home, r_b.at[h]).start()

                @pl.when(jnp.logical_not(mine))
                def _():
                    remote(bbuf.at[h, s], home, s_b.at[h], r_b.at[h], mine_at(4 * (s // 2) + 2 + s % 2)).start()

    def backward(finish):
        @pl.when(is_k)
        def _():
            for h in range(2):
                await_bytes(kbuf.at[h], r_b.at[h])
                d = jnp.concatenate([kbuf[h, pl.ds(a, 48, stride=8), :] for a in range(8)], axis=1)
                term = dot(tzb[h], pieces(d, 0))
                acc[...] = acc[...] + term if h else term
            for a in range(8):
                f = acc[:64, 128 * a : 128 * a + 128] - sign * swap(acc[64:, 128 * a : 128 * a + 128])
                finish(a, kin[a] * cur[a] + inside[a] * f)
            for h in range(2):
                await_bytes(sbuf.at[h, pl.ds(0, 24 * (MEMBERS - 1))], s_f.at[h])
                await_bytes(bbuf.at[h, pl.ds(0, HOLDERS - 1)], s_b.at[h])

        @pl.when(jnp.logical_not(is_k))
        def _():
            for h in range(2):
                await_bytes(bbuf.at[h], s_b.at[h])

    center = 0.5 * (upper_ref[0] + lower_ref[0])
    half_width = 0.5 * (upper_ref[0] - lower_ref[0])

    def step(k, _):
        forward()
        middle(k == 0)
        alpha = jnp.where(k == 0, 1.0, 2.0).astype(F32)
        beta = jnp.where(k == 0, 0.0, 1.0).astype(F32)

        def finish(a, h):
            old = cur[a]
            new = alpha * (h - center * old) / half_width - beta * prev[a]
            prev[a] = old
            cur[a] = new

        backward(finish)
        return 0

    lax.fori_loop(0, 3, step, 0)

    on_zero = core == 0
    summing = both(on_zero, active)

    def for_rows(do):
        @pl.when(is_k)
        def _():
            for a in range(8):
                held, kx = kx_of_slot(a)
                home, jj = quot(kx, 3), mod(kx, 3)

                @pl.when(held)
                def _():
                    for n in range(4):
                        do(a, n, jj, dev(2 * n, home))

    def scatter(src, w):
        def one(a, n, jj, target):
            dst = gy.at[w, pl.ds(pl.multiple_of(256 * jj + 16 * band, 8), 16)]
            remote(src.at[a, pl.ds(16 * n, 16)], dst, s_g.at[w, 4 * a + n], r_g.at[w], target).start()

        for_rows(one)

    def scattered(src, w):
        def one(a, n, jj, target):
            await_bytes(src.at[a, pl.ds(16 * n, 16)], s_g.at[w, 4 * a + n])

        for_rows(one)

    def all_rows(w):
        @pl.when(lone)
        def _():
            await_bytes(gy.at[w, pl.ds(0, 256)], r_g.at[w])

        @pl.when(jnp.logical_not(lone))
        def _():
            await_bytes(gy.at[w], r_g.at[w])

        rows = []
        for jj in range(3):
            for r in range(16):
                x = gy[w, pl.ds(256 * jj + r, BANDS, stride=16), :]
                rows.append(jnp.where(lone, 0.0, x) if jj else x)
        a = jnp.concatenate(rows, axis=1)
        b = jnp.concatenate([-sign * swap(x) for x in rows], axis=1)
        return jnp.concatenate([a, b], axis=0)

    my_slot = jnp.minimum(jnp.where(i <= 8, i, jnp.maximum(i - 15, 0)), 16)

    def added(terms):
        while len(terms) > 1:
            terms = [a + b for a, b in zip(terms[::2], terms[1::2])] + ([terms[-1]] if len(terms) % 2 else [])
        return terms[0]

    lane2 = lax.broadcasted_iota(jnp.int32, (16, 128), 1)

    def inverse_rows(g):
        row = lax.broadcasted_iota(jnp.int32, (32, 128), 0)
        ln = lax.broadcasted_iota(jnp.int32, (32, 128), 1)
        top = jnp.where(lane2 < 16, g, -g)
        bottom = jnp.where(lane2 < 16, pltpu.roll(g, 112, 1), pltpu.roll(g, 16, 1))
        m = jnp.where(ln < 32, jnp.concatenate([top, bottom], 0), 0.0)
        m = m + jnp.where(ln == row + 32, 1.0, 0.0)
        for j in range(32):
            pivot = m[j : j + 1, :]
            factor = m[:, j : j + 1] * (1.0 / pivot[:, j : j + 1])
            m = m - jnp.where(row > j, factor, 0.0) * pivot
        diag = jnp.sum(jnp.where(ln == row, m, 0.0), axis=1, keepdims=True)
        u = m[:16] / jnp.sqrt(diag[:16])
        return jnp.where(lane2 < 32, pltpu.roll(u, 96, 1), 0.0)

    pl.semaphore_wait(planes_in, 15)
    scatter(cur, 0)
    forward()
    middle(False)

    def keep(a, h):
        hy[a] = h

    backward(keep)
    scatter(hy, 1)

    @pl.when(summing)
    def _():
        high, low = split(all_rows(0))
        bh[...] = high
        bl[...] = low
        g = (dot_t(bh[:BANDS], high) + dot_t(bh[:BANDS], low) + dot_t(bl[:BANDS], high)) * (1.0 / CELLS)
        g = jnp.concatenate([g, jnp.zeros((BANDS, 96), F32)], axis=1)
        packed = g[0:4]
        for n in range(1, 4):
            packed = packed + pltpu.roll(g[4 * n : 4 * n + 4], 32 * n, 1)
        part[...] = packed
        full[17 * y + my_slot] = packed
        for n in range(4):
            for ii in ACTIVE:

                @pl.when(jnp.logical_not(is_me(dev(2 * n, ii))))
                def _():
                    remote(
                        part, full.at[17 * y + my_slot], s_p.at[0], r_p.at[0], dev(2 * n, ii)
                    ).start()

        await_bytes(full.at[pl.ds(0, 67)], r_p.at[0])
        total = added([full[n] for n in range(68)])

        g = jnp.concatenate([total] + [pltpu.roll(total, 128 - 32 * n, 1) for n in range(1, 4)], axis=0)
        u_rows = inverse_rows(jnp.where(lane2 < 32, g, 0.0))
        w_high, w_low = split(jnp.where(lane2 < 16, u_rows, -u_rows)[:, :32])

        def rotated(high, low):
            return dot(w_high, high) + dot(w_high, low) + dot(w_low, high)

        q = rotated(bh[...], bl[...])
        for n in range(48):
            qs[pl.ds(n, BANDS, stride=48), :] = q[:, 128 * n : 128 * n + 128]
        hq = rotated(*split(all_rows(1)))
        e = q[:, :128] * hq[:, :128]
        for n in range(1, 48):
            e = e + q[:, 128 * n : 128 * n + 128] * hq[:, 128 * n : 128 * n + 128]
        e = jnp.sum(e, axis=1, keepdims=True) * (1.0 / CELLS)
        row = lax.broadcasted_iota(jnp.int32, (16, 128), 0)
        epart[...] = jnp.sum(jnp.where(lane2 == row, e, 0.0), axis=0, keepdims=True)
        mine = 17 * y + my_slot
        efull[mine] = epart[...]
        for pp in range(8):
            for n in range(32):
                ii = mod(i + 4 + n, 32)

                def send():
                    remote(epart, efull.at[mine], s_p.at[1], r_p.at[1], dev(pp, ii)).start()

                if n == 28:
                    pl.when(p != pp)(send)
                else:
                    send()

        for t in range(8):
            src = qs.at[pl.ds(96 * t, 96)]

            @pl.when(p == t)
            def _():
                pltpu.make_async_copy(src, ob.at[y], r_o.at[0]).start()

            @pl.when(p != t)
            def _():
                remote(src, ob.at[y], s_o.at[t], r_o.at[0], dev(t, i)).start()

    @pl.when(active)
    def _():
        await_bytes(ob, r_o.at[0])
        zero = jnp.zeros((64, 128), F32)
        low_lanes, high_lanes = lane < 25, jnp.logical_and(lane >= 72, lane < 96)
        for k in range(6):
            j, jj = k // 3, k % 3
            rows = jnp.concatenate([ob[n, 16 * k : 16 * k + 16, :] for n in range(4)] + [zero], axis=0)
            if jj:
                rows = jnp.where(lone, 0.0, rows)
            rows = rows.T
            rows = jnp.where(low_lanes, rows, jnp.where(high_lanes, pltpu.roll(rows, 47, 1), 0.0))
            for c in range(2):
                grid[c, 0:25] = rows[64 * c : 64 * c + 25]
                grid[c, 25:72] = jnp.zeros((47, 128), F32)
                grid[c, 72:96] = rows[64 * c + 25 : 64 * c + BOX]
                thirds = pack(*(grid[c, pl.ds(r, 24, stride=4), :] for r in range(4)))
                for t in range(3):
                    xin[3 * c + jj, pl.ds(2 * t + j, 24, stride=6), :] = thirds[t]

    @pl.when(jnp.logical_not(active))
    def _():
        xin[...] = jnp.zeros((6, 144, 128), F32)

    pltpu.make_async_copy(xin, out_hbm, s_out.at[0]).start()

    for k in range(6):
        valid, _, target = start_of(k)

        @pl.when(both(valid, jnp.logical_not(is_me(target))))
        def _():
            await_bytes(xt.at[k], s_init.at[k])

    for n in range(2):

        @pl.when(jnp.logical_not(is_me(v_target(n))))
        def _():
            await_bytes(vp, s_v.at[n])

    scattered(cur, 0)
    scattered(hy, 1)

    @pl.when(summing)
    def _():
        await_bytes(sbuf.at[0, pl.ds(0, 255)], s_p.at[1])
        await_bytes(full.at[pl.ds(0, 67)], s_p.at[0])
        for t in range(8):

            @pl.when(p != t)
            def _():
                await_bytes(qs.at[pl.ds(96 * t, 96)], s_o.at[t])

    await_bytes(xin, s_out.at[0])

    @pl.when(summing)
    def _():
        await_bytes(efull.at[pl.ds(0, 67)], r_p.at[1])

    @pl.when(jnp.logical_not(summing))
    def _():
        await_bytes(efull, r_p.at[1])

    e = added([efull[n] for n in range(68)])
    energy_ref[...] = pltpu.roll(e, 128 - 2 * p, 1)[:, :2]
    weights = jax.nn.sigmoid((fermi_ref[0] - e) / TEMPER)
    weighted = jnp.where(lane < BANDS, weights * e, 0.0)
    band_energy_ref[...] = jnp.sum(weighted, axis=1, keepdims=True) / float(BANDS)


def call(lower, upper, fermi, height, x, v):
    smem = pl.BlockSpec(memory_space=pltpu.SMEM)
    hbm = pl.BlockSpec(memory_space=pl.ANY)
    vmem = pl.BlockSpec(memory_space=pltpu.VMEM)
    sem = pltpu.SemaphoreType.DMA
    consts = tables()

    def buf(*shape):
        return pltpu.VMEM(shape, F32)

    return pl.pallas_call(
        kernel,
        out_shape=(
            jax.ShapeDtypeStruct((6, 144, 128), F32),
            jax.ShapeDtypeStruct((1, 2), F32),
            jax.ShapeDtypeStruct((1, 1), F32),
        ),
        in_specs=[smem] * 3 + [hbm] * 9,
        out_specs=(hbm, vmem, vmem),
        scratch_shapes=[
            buf(6, 144, 128),
            buf(2, 96, 128),
            pltpu.VMEM((3, 96), jnp.int32),
            buf(3, 96, 96),
            buf(3, 72, 128),
            buf(6, 72, 128),
            buf(6, 96, 128),
            buf(128, 1024),
            *[pltpu.VMEM(t.shape, BF16) for t in consts],
            buf(6, 56, 128),
            buf(8, 56, 128),
            buf(8, 64, 128),
            buf(8, 64, 128),
            buf(8, 64, 128),
            buf(8, 64, 128),
            buf(8, 64, 128),
            buf(2, 384, 128),
            buf(2, 7, 24, 128),
            buf(2, 7, 24, 128),
            buf(2, 384, 128),
            buf(2, 768, 128),
            pltpu.VMEM((32, 6144), BF16),
            pltpu.VMEM((32, 6144), BF16),
            buf(4, 128),
            buf(68, 4, 128),
            buf(1, 128),
            buf(68, 1, 128),
            buf(768, 128),
            buf(4, 96, 128),
            sem((3,)),
            sem((1,)),
            sem((6,)),
            sem((6,)),
            sem((8,)),
            sem((4,)),
            sem((2,)),
            sem((2,)),
            sem((2,)),
            sem((2,)),
            sem((2,)),
            sem((2, 32)),
            sem((2,)),
            sem((2,)),
            sem((2,)),
            sem((8,)),
            sem((1,)),
            pltpu.SemaphoreType.REGULAR,
        ],
        compiler_params=pltpu.CompilerParams(
            has_side_effects=True, collective_id=0, vmem_limit_bytes=60 * 2**20
        ),
    )(lower, upper, fermi, height, x, v, *[jnp.asarray(t) for t in consts])


def local(start_bands, potential, half_height, lower_bound, upper_bound, fermi_level):
    x = start_bands.reshape(2, 2, 3, 72, 128).transpose(0, 2, 3, 1, 4).reshape(6, 144, 128)
    v = potential.transpose(2, 0, 1)
    out, energies, band_energy = call(lower_bound, upper_bound, fermi_level, half_height, x, v)
    out = out.reshape(2, 3, 72, 2, 128).transpose(0, 3, 1, 2, 4).reshape(2, 2, 3, NG * NG)
    return out, energies.reshape(2), band_energy.reshape(1)


def solution(mesh):
    placed = (P(None, "band", "fft", None), P(None, None, "fft"), P("fft", None), P(), P(), P())
    return jax.shard_map(
        local,
        mesh=mesh,
        in_specs=placed,
        out_specs=(P(None, "band", "fft", None), P("band"), P()),
        check_vma=False,
    )
```

```python
import math

import jax
import jax.numpy as jnp
import ml_dtypes
import numpy as np
from jax import lax
from jax.experimental import pallas as pl
from jax.experimental.pallas import tpu as pltpu
from jax.sharding import PartitionSpec as P

NG = 96
CELLS = float(NG**3)
BOX = 49
KIN = 12.0 / 24**2
TEMPER = 0.5
BANDS = 16
FAR_FIRST = (7, 6, 5, 3, 4, 2, 1, 0)
ACTIVE = (*range(9), *range(24, 32))
MEMBERS = 16
HOLDERS = 7
ZP = 3
F32, BF16 = jnp.float32, jnp.bfloat16
MESH = pl.DeviceIdType.MESH


def box_frequency():
    r = np.arange(BOX)
    return np.where(r <= 24, r, r - BOX)


def halves(table):
    table = table.astype(np.float32)
    high = table.astype(ml_dtypes.bfloat16)
    low = (table - high.astype(np.float32)).astype(ml_dtypes.bfloat16)
    return high, low


def tables():
    freq = box_frequency()
    angle = 2.0 * math.pi / NG * ((np.arange(NG)[:, None] * freq[None, :]) % NG)
    cosine, sine = np.cos(angle), np.sin(angle)
    ahead = np.zeros((192, 64))
    ahead[:96, :BOX], ahead[96:, :BOX] = cosine, sine
    back = np.zeros((128, 96))
    back[:BOX], back[64 : 64 + BOX] = cosine.T, sine.T
    lanes = np.zeros((128, 256))
    lanes[:BOX, :96], lanes[:BOX, 128:224] = cosine.T, sine.T
    lanes[64 : 64 + BOX, :96], lanes[64 : 64 + BOX, 128:224] = -sine.T, cosine.T
    lanes_back = lanes.T.copy()
    plane = np.arange(NG).reshape(MEMBERS, 2, ZP)

    def left(t):
        high, low = halves(t)
        return np.concatenate([high, high, low], axis=1)

    def right(t):
        high, low = halves(t)
        return np.concatenate([high, high, low], axis=0)

    z_ahead = [np.concatenate([ahead[plane[:, h].ravel()], ahead[96 + plane[:, h].ravel()]]) for h in range(2)]
    z_back = [back[:, plane[:, h].ravel()] for h in range(2)]
    return (
        np.stack([left(t) for t in z_ahead]),
        left(ahead),
        np.stack([left(t) for t in z_back]),
        left(back),
        right(lanes),
        right(lanes_back),
    )


def split(x):
    high = x.astype(BF16)
    return high, (x - high.astype(F32)).astype(BF16)


def pieces(x, axis):
    high, low = split(x)
    return jnp.concatenate([high, low, high], axis=axis)


def dot(a, b):
    return jnp.dot(a, b, preferred_element_type=F32)


def dot_t(a, b):
    return lax.dot_general(a, b, (((1,), (1,)), ((), ())), preferred_element_type=F32)


def kernel(
    lower_ref,
    upper_ref,
    fermi_ref,
    height_hbm,
    x_hbm,
    v_hbm,
    tz_hbm,
    tx_hbm,
    tzb_hbm,
    txb_hbm,
    ty_hbm,
    tyb_hbm,
    out_hbm,
    energy_ref,
    band_energy_ref,
    xin,
    grid,
    height_ref,
    vin,
    vp,
    vb,
    vfull,
    acc,
    tz,
    tx,
    tzb,
    txb,
    ty,
    tyb,
    xt,
    x0,
    cur,
    prev,
    hy,
    inside,
    kin,
    sbuf,
    rbuf,
    bbuf,
    kbuf,
    gy,
    bh,
    bl,
    part,
    full,
    epart,
    efull,
    qs,
    ob,
    s_in,
    s_out,
    s_t,
    s_init,
    r_init,
    s_v,
    r_v,
    s_f,
    r_f,
    s_b,
    r_b,
    s_g,
    r_g,
    s_p,
    r_p,
    s_o,
    r_o,
    planes_in,
):
    p = lax.axis_index("band")
    i = lax.axis_index("fft")

    def quot(a, n):
        return a // n if isinstance(a, int) else lax.div(a, jnp.int32(n))

    def mod(a, n):
        return a % n if isinstance(a, int) else lax.rem(a, jnp.int32(n))

    def both(a, b):
        return jnp.logical_and(a, b)

    y, core = quot(p, 2), mod(p, 2)
    y2, yl = quot(y, 2), mod(y, 2)
    gx, gzz = quot(i, 8), mod(i, 8)
    x2, xl = quot(gx, 2), mod(gx, 2)
    gz, zl = quot(gzz, 2), mod(gzz, 2)
    band = 8 * y2 + 4 * x2 + gz
    xr = 2 * yl + mod(xl + yl, 2)
    zr = 2 * core + mod(zl + core, 2)
    place = 4 * xr + zr
    me = 4 * mod(xr + 2 * x2, 4) + mod(zr + 2 * quot(gz, 2), 4)
    chip = 2 * xr + zr - 2
    is_k = both(core == 1, chip < HOLDERS)
    active = jnp.logical_or(i <= 8, i >= 24)
    lone = i == 8

    def dev(pp, ii):
        return {"band": pp, "fft": ii}

    def at_place(yy, xx, zz, xr_, zr_):
        c = quot(zr_, 2)
        return dev(
            4 * yy + 2 * quot(xr_, 2) + c,
            16 * xx + 8 * mod(quot(xr_ + 1, 2), 2) + 2 * zz + mod(quot(zr_ + 1, 2), 2),
        )

    def holder(b, s):
        return at_place(quot(b, 8), mod(quot(b, 4), 2), mod(b, 4), quot(s, 2), 2 + mod(s, 2))

    def mine_at(n):
        return at_place(y2, x2, gz, n // 4, n % 4)

    def across(d, c):
        yy, xx, zz = mod(yl + d // 4, 2), mod(xl + d // 2 % 2, 2), mod(zl + d % 2, 2)
        return (
            2 * yy + mod(xx + yy, 2),
            2 * c + mod(zz + c, 2),
            dev(4 * y2 + 2 * yy + c, 16 * x2 + 8 * xx + 2 * gz + zz),
        )

    def is_me(where):
        return both(where["band"] == p, where["fft"] == i)

    def remote(src, dst, ss, rs, where):
        return pltpu.make_async_remote_copy(
            src_ref=src, dst_ref=dst, send_sem=ss, recv_sem=rs, device_id=where, device_id_type=MESH
        )

    def await_bytes(ref, sem):
        pltpu.make_async_copy(ref, ref, sem).wait()

    for src, dst, n in ((x_hbm, xin, 0), (v_hbm, vin, 1), (height_hbm, height_ref, 2)):
        pltpu.make_async_copy(src, dst, s_in.at[n]).start()
    for n, (src, dst) in enumerate(
        ((tz_hbm, tz), (tx_hbm, tx), (tzb_hbm, tzb), (txb_hbm, txb), (ty_hbm, ty), (tyb_hbm, tyb))
    ):
        pltpu.make_async_copy(src, dst, s_t.at[n]).start()

    barrier = pltpu.get_barrier_semaphore()

    def tell(where):
        pl.semaphore_signal(barrier, inc=1, device_id=where, device_id_type=MESH)

    def kx_of_slot(a):
        q = 8 * chip + a
        return q < BOX, jnp.where(q <= 24, q, q + 47)

    @pl.when(is_k)
    def _():
        for a in range(8):
            held, kx = kx_of_slot(a)
            native = dev(quot(band, 2), quot(kx, 3))

            @pl.when(both(held, jnp.logical_not(is_me(native))))
            def _():
                tell(native)

    for h in range(2):
        source = dev(2 * y + quot(gz, 2), 2 * me + h)

        @pl.when(jnp.logical_not(is_me(source)))
        def _():
            tell(source)

    for n in range(MEMBERS):

        @pl.when(place != n)
        def _():
            tell(mine_at(n))

    def counterpart(n):
        return at_place(
            mod(y2 + n // 8, 2), mod(x2 + (n // 4) % 2, 2), mod(gz + n % 4, 4), xr, zr
        )

    for n in range(1, 16):
        tell(counterpart(n))

    def start_of(k):
        j, jj = k // 3, k % 3
        kx = 3 * i + jj
        valid = jnp.logical_or(kx <= 24, kx >= 72)
        q = jnp.where(kx <= 24, kx, kx - 47)
        s = jnp.minimum(jnp.maximum(quot(q, 8), 0), HOLDERS - 1)
        return valid, mod(q, 8), holder(2 * p + j, s)

    def v_target(n):
        xx = mod(quot(gx, 2) + yl, 2)
        return at_place(y2, xx, 2 * core + n, mod(gx + 2 * xx, 4), mod(quot(gzz, 2) + 2 * core, 4))

    expected = jnp.int32(30)
    for k in range(6):
        valid, _, target = start_of(k)
        expected = expected + both(valid, jnp.logical_not(is_me(target))).astype(jnp.int32)
    for n in range(2):
        expected = expected + jnp.logical_not(is_me(v_target(n))).astype(jnp.int32)

    lane = lax.broadcasted_iota(jnp.int32, (1, 128), 1)
    sign = jnp.where(lane < 64, -1.0, 1.0).astype(F32)

    def swap(x):
        return pltpu.roll(x, 64, 1)

    def boxed_lanes(x):
        return jnp.where(lane < 25, x, jnp.where(lane < BOX, pltpu.roll(x, 128 - 47, 1), 0.0))

    def unpack(t0, t1, t2):
        return (
            t0,
            jnp.where(lane < 32, pltpu.roll(t0, 32, 1), pltpu.roll(t1, 32, 1)),
            jnp.where(lane < 64, pltpu.roll(t1, 64, 1), pltpu.roll(t2, 64, 1)),
            pltpu.roll(t2, 96, 1),
        )

    def pack(o0, o1, o2, o3):
        return (
            jnp.where(lane < 96, o0, pltpu.roll(o1, 96, 1)),
            jnp.where(lane < 64, pltpu.roll(o1, 96, 1), pltpu.roll(o2, 64, 1)),
            jnp.where(lane < 32, pltpu.roll(o2, 64, 1), pltpu.roll(o3, 32, 1)),
        )

    await_bytes(xin, s_in.at[0])
    await_bytes(height_ref, s_in.at[2])
    for k in range(6):
        j, jj = k // 3, k % 3
        for c in range(2):
            quarter = unpack(*(xin[3 * c + jj, pl.ds(2 * t + j, 24, stride=6), :] for t in range(3)))
            for r in range(4):
                grid[c, pl.ds(r, 24, stride=4), :] = boxed_lanes(quarter[r])
        pad = jnp.zeros((15, 128), F32)
        rows = jnp.concatenate([grid[0, 0:25], grid[0, 72:96], pad, grid[1, 0:25], grid[1, 72:96], pad], axis=0)
        xt[k] = rows.T[:56]
    for jj in range(3):
        h = height_ref[jj : jj + 1, :].astype(F32)
        h = boxed_lanes(jnp.concatenate([h, jnp.zeros((1, 32), F32)], axis=1))
        h = jnp.where(lane < BOX, h, -1.0)
        h = jnp.where(lane < 64, h, pltpu.roll(h, 64, 1))
        for j in range(2):
            xt[3 * j + jj, BOX : BOX + 1, :] = h
    await_bytes(vin, s_in.at[1])
    for z in range(3):
        grid[0] = jnp.concatenate([vin[z], jnp.zeros((96, 32), F32)], axis=1)
        thirds = pack(*(grid[0, pl.ds(r, 24, stride=4), :] for r in range(4)))
        for t in range(3):
            vp[z, 24 * t : 24 * t + 24, :] = thirds[t]

    pl.semaphore_wait(barrier, expected)

    for k in range(6):
        valid, slot, target = start_of(k)

        @pl.when(both(valid, is_me(target)))
        def _():
            pltpu.make_async_copy(xt.at[k], x0.at[slot], r_init.at[slot]).start()

        @pl.when(both(valid, jnp.logical_not(is_me(target))))
        def _():
            remote(xt.at[k], x0.at[slot], s_init.at[k], r_init.at[slot], target).start()

    for n in range(2):
        target = v_target(n)
        home = vb.at[pl.ds(3 * mod(i, 2), 3)]

        @pl.when(is_me(target))
        def _():
            pltpu.make_async_copy(vp, home, r_v.at[mod(i, 2)]).start()

        @pl.when(jnp.logical_not(is_me(target)))
        def _():
            remote(vp, home, s_v.at[n], r_v.at[mod(i, 2)], target).start()

    for n in range(1, 16):
        pl.semaphore_signal(planes_in, inc=1, device_id=counterpart(n), device_id_type=MESH)

    for n, dst in enumerate((tz, tx, tzb, txb, ty, tyb)):
        await_bytes(dst, s_t.at[n])

    @pl.when(is_k)
    def _():
        row = lax.broadcasted_iota(jnp.int32, (64, 128), 0)
        col_ = lax.broadcasted_iota(jnp.int32, (64, 128), 1) % 64
        fz = jnp.where(row <= 24, row, row - BOX)
        fy = jnp.where(col_ <= 24, col_, col_ - BOX)
        in_box = jnp.logical_and(row < BOX, col_ < BOX)
        yz = (fz * fz + fy * fy).astype(F32)
        absz = jnp.abs(fz).astype(F32)

        def plane(a, _):
            q = 8 * chip + a

            @pl.when(q < BOX)
            def _():
                await_bytes(x0.at[a], r_init.at[a])
                fx = jnp.where(q <= 24, q, q - BOX)
                data = x0[a]
                data = jnp.concatenate([data, jnp.zeros((8, 128), F32)], axis=0)
                keep = both(in_box, absz <= data[BOX : BOX + 1])
                cur[a] = jnp.where(keep, data, 0.0)
                inside[a] = jnp.where(keep, 1.0 / CELLS, 0.0)
                kin[a] = jnp.where(keep, KIN * (yz + (fx * fx).astype(F32)), 0.0)

            @pl.when(q >= BOX)
            def _():
                zero = jnp.zeros((64, 128), F32)
                cur[a] = zero
                inside[a] = zero
                kin[a] = zero

            prev[a] = jnp.zeros((64, 128), F32)
            return 0

        lax.fori_loop(0, 8, plane, 0)

    def message(m):
        return pl.ds(pl.multiple_of(24 * m, 8), 24)

    def forward():
        @pl.when(is_k)
        def _():
            x = pieces(jnp.concatenate([cur[a] for a in range(8)], axis=1), 0)
            for h in range(2):
                out = dot(tz[h], x)
                for a in range(8):
                    c, s = out[:48, 128 * a : 128 * a + 128], out[48:, 128 * a : 128 * a + 128]
                    sbuf[h, pl.ds(a, 48, stride=8), :] = c + sign * swap(s)

                home = rbuf.at[h, chip]
                for d in FAR_FIRST:
                    for c in range(2):
                        xr_, zr_, target = across(d, c)
                        slab = 4 * mod(xr_ + 2 * x2, 4) + mod(zr_ + 2 * quot(gz, 2), 4)
                        src = sbuf.at[h, message(slab)]
                        if d == 0 and c == 1:
                            pltpu.make_async_copy(src, home, r_f.at[h]).start()
                        else:
                            remote(src, home, s_f.at[h], r_f.at[h], target).start()

    def middle(first):
        zero8 = jnp.zeros((8, 128), F32)
        for h in range(2):
            await_bytes(rbuf.at[h], r_f.at[h])
            d = jnp.concatenate(
                [
                    jnp.concatenate(
                        [rbuf[h, s, 8 * z : 8 * z + 8, :] for s in range(HOLDERS)] + [zero8], axis=0
                    )
                    for z in range(ZP)
                ],
                axis=1,
            )
            out = dot(tx[...], pieces(d, 0))
            rows = jnp.concatenate(
                [
                    out[:96, 128 * z : 128 * z + 128] + sign * swap(out[96:, 128 * z : 128 * z + 128])
                    for z in range(ZP)
                ],
                axis=0,
            )
            psi = dot(pieces(rows, 1), ty[...])

            @pl.when(first)
            def _():
                await_bytes(vb.at[pl.ds(3 * h, 3)], r_v.at[h])
                for z in range(3 * h, 3 * h + 3):
                    quarter = unpack(*(vb[z, 24 * t : 24 * t + 24, :] for t in range(3)))
                    for r in range(4):
                        vfull[z, pl.ds(r, 24, stride=4), :] = jnp.where(lane < NG, quarter[r], 0.0)

            v = jnp.concatenate([vfull[3 * h + z] for z in range(ZP)], axis=0)
            psi = psi * jnp.concatenate([v, v], axis=1)
            rows = dot(pieces(psi, 1), tyb[...])
            d = jnp.concatenate([rows[96 * z : 96 * z + 96] for z in range(ZP)], axis=1)
            out = dot(txb[...], pieces(d, 0))
            for z in range(ZP):
                o = out[:64, 128 * z : 128 * z + 128] - sign * swap(out[64:, 128 * z : 128 * z + 128])
                for s in range(HOLDERS):
                    bbuf[h, s, 8 * z : 8 * z + 8, :] = o[8 * s : 8 * s + 8]

            home = kbuf.at[h, message(me)]
            for d in FAR_FIRST:
                xr_, zr_, target = across(d, 1)
                s = 2 * xr_ + zr_ - 2
                src = bbuf.at[h, jnp.minimum(s, HOLDERS - 1)]
                held = s < HOLDERS
                if d == 0:

                    @pl.when(is_k)
                    def _():
                        pltpu.make_async_copy(src, home, r_b.at[h]).start()

                    held = both(held, core == 0)

                @pl.when(held)
                def _():
                    remote(src, home, s_b.at[h], r_b.at[h], target).start()

    def backward(finish):
        @pl.when(is_k)
        def _():
            for h in range(2):
                await_bytes(kbuf.at[h], r_b.at[h])
                d = jnp.concatenate([kbuf[h, pl.ds(a, 48, stride=8), :] for a in range(8)], axis=1)
                term = dot(tzb[h], pieces(d, 0))
                acc[...] = acc[...] + term if h else term
            for a in range(8):
                f = acc[:64, 128 * a : 128 * a + 128] - sign * swap(acc[64:, 128 * a : 128 * a + 128])
                finish(a, kin[a] * cur[a] + inside[a] * f)
            for h in range(2):
                await_bytes(sbuf.at[h, pl.ds(0, 24 * (MEMBERS - 1))], s_f.at[h])
                await_bytes(bbuf.at[h, pl.ds(0, HOLDERS - 1)], s_b.at[h])

        @pl.when(jnp.logical_not(is_k))
        def _():
            for h in range(2):
                await_bytes(bbuf.at[h], s_b.at[h])

    center = 0.5 * (upper_ref[0] + lower_ref[0])
    half_width = 0.5 * (upper_ref[0] - lower_ref[0])

    def step(k, _):
        forward()
        middle(k == 0)
        alpha = jnp.where(k == 0, 1.0, 2.0).astype(F32)
        beta = jnp.where(k == 0, 0.0, 1.0).astype(F32)

        def finish(a, h):
            old = cur[a]
            new = alpha * (h - center * old) / half_width - beta * prev[a]
            prev[a] = old
            cur[a] = new

        backward(finish)
        return 0

    lax.fori_loop(0, 3, step, 0)

    on_zero = core == 0
    summing = both(on_zero, active)

    def for_rows(do):
        @pl.when(is_k)
        def _():
            for a in range(8):
                held, kx = kx_of_slot(a)
                home, jj = quot(kx, 3), mod(kx, 3)

                @pl.when(held)
                def _():
                    for n in range(4):
                        do(a, n, jj, dev(2 * n, home))

    def scatter(src, w):
        def one(a, n, jj, target):
            dst = gy.at[w, pl.ds(pl.multiple_of(256 * jj + 16 * band, 8), 16)]
            remote(src.at[a, pl.ds(16 * n, 16)], dst, s_g.at[w, 4 * a + n], r_g.at[w], target).start()

        for_rows(one)

    def scattered(src, w):
        def one(a, n, jj, target):
            await_bytes(src.at[a, pl.ds(16 * n, 16)], s_g.at[w, 4 * a + n])

        for_rows(one)

    def all_rows(w):
        @pl.when(lone)
        def _():
            await_bytes(gy.at[w, pl.ds(0, 256)], r_g.at[w])

        @pl.when(jnp.logical_not(lone))
        def _():
            await_bytes(gy.at[w], r_g.at[w])

        rows = []
        for jj in range(3):
            for r in range(16):
                x = gy[w, pl.ds(256 * jj + r, BANDS, stride=16), :]
                rows.append(jnp.where(lone, 0.0, x) if jj else x)
        a = jnp.concatenate(rows, axis=1)
        b = jnp.concatenate([-sign * swap(x) for x in rows], axis=1)
        return jnp.concatenate([a, b], axis=0)

    my_slot = jnp.minimum(jnp.where(i <= 8, i, jnp.maximum(i - 15, 0)), 16)

    def added(terms):
        while len(terms) > 1:
            terms = [a + b for a, b in zip(terms[::2], terms[1::2])] + ([terms[-1]] if len(terms) % 2 else [])
        return terms[0]

    lane2 = lax.broadcasted_iota(jnp.int32, (16, 128), 1)

    def inverse_rows(g):
        row = lax.broadcasted_iota(jnp.int32, (32, 128), 0)
        ln = lax.broadcasted_iota(jnp.int32, (32, 128), 1)
        top = jnp.where(lane2 < 16, g, -g)
        bottom = jnp.where(lane2 < 16, pltpu.roll(g, 112, 1), pltpu.roll(g, 16, 1))
        m = jnp.where(ln < 32, jnp.concatenate([top, bottom], 0), 0.0)
        m = m + jnp.where(ln == row + 32, 1.0, 0.0)
        for j in range(32):
            pivot = m[j : j + 1, :]
            factor = m[:, j : j + 1] * (1.0 / pivot[:, j : j + 1])
            m = m - jnp.where(row > j, factor, 0.0) * pivot
        diag = jnp.sum(jnp.where(ln == row, m, 0.0), axis=1, keepdims=True)
        u = m[:16] / jnp.sqrt(diag[:16])
        return jnp.where(lane2 < 32, pltpu.roll(u, 96, 1), 0.0)

    pl.semaphore_wait(planes_in, 15)
    scatter(cur, 0)
    forward()
    middle(False)

    def keep(a, h):
        hy[a] = h

    backward(keep)
    scatter(hy, 1)

    @pl.when(summing)
    def _():
        high, low = split(all_rows(0))
        bh[...] = high
        bl[...] = low
        g = (dot_t(bh[:BANDS], high) + dot_t(bh[:BANDS], low) + dot_t(bl[:BANDS], high)) * (1.0 / CELLS)
        g = jnp.concatenate([g, jnp.zeros((BANDS, 96), F32)], axis=1)
        packed = g[0:4]
        for n in range(1, 4):
            packed = packed + pltpu.roll(g[4 * n : 4 * n + 4], 32 * n, 1)
        part[...] = packed
        full[17 * y + my_slot] = packed
        for n in range(4):
            for ii in ACTIVE:

                @pl.when(jnp.logical_not(is_me(dev(2 * n, ii))))
                def _():
                    remote(
                        part, full.at[17 * y + my_slot], s_p.at[0], r_p.at[0], dev(2 * n, ii)
                    ).start()

        await_bytes(full.at[pl.ds(0, 67)], r_p.at[0])
        total = added([full[n] for n in range(68)])

        g = jnp.concatenate([total] + [pltpu.roll(total, 128 - 32 * n, 1) for n in range(1, 4)], axis=0)
        u_rows = inverse_rows(jnp.where(lane2 < 32, g, 0.0))
        w_high, w_low = split(jnp.where(lane2 < 16, u_rows, -u_rows)[:, :32])

        def rotated(high, low):
            return dot(w_high, high) + dot(w_high, low) + dot(w_low, high)

        q = rotated(bh[...], bl[...])
        for n in range(48):
            qs[pl.ds(n, BANDS, stride=48), :] = q[:, 128 * n : 128 * n + 128]
        hq = rotated(*split(all_rows(1)))
        e = q[:, :128] * hq[:, :128]
        for n in range(1, 48):
            e = e + q[:, 128 * n : 128 * n + 128] * hq[:, 128 * n : 128 * n + 128]
        e = jnp.sum(e, axis=1, keepdims=True) * (1.0 / CELLS)
        row = lax.broadcasted_iota(jnp.int32, (16, 128), 0)
        epart[...] = jnp.sum(jnp.where(lane2 == row, e, 0.0), axis=0, keepdims=True)
        mine = 17 * y + my_slot
        efull[mine] = epart[...]
        for pp in range(8):
            for n in range(32):
                ii = mod(i + 4 + n, 32)

                def send():
                    remote(epart, efull.at[mine], s_p.at[1], r_p.at[1], dev(pp, ii)).start()

                if n == 28:
                    pl.when(p != pp)(send)
                else:
                    send()

        for t in range(8):
            src = qs.at[pl.ds(96 * t, 96)]

            @pl.when(p == t)
            def _():
                pltpu.make_async_copy(src, ob.at[y], r_o.at[0]).start()

            @pl.when(p != t)
            def _():
                remote(src, ob.at[y], s_o.at[t], r_o.at[0], dev(t, i)).start()

    @pl.when(active)
    def _():
        await_bytes(ob, r_o.at[0])
        zero = jnp.zeros((64, 128), F32)
        low_lanes, high_lanes = lane < 25, jnp.logical_and(lane >= 72, lane < 96)
        for k in range(6):
            j, jj = k // 3, k % 3
            rows = jnp.concatenate([ob[n, 16 * k : 16 * k + 16, :] for n in range(4)] + [zero], axis=0)
            if jj:
                rows = jnp.where(lone, 0.0, rows)
            rows = rows.T
            rows = jnp.where(low_lanes, rows, jnp.where(high_lanes, pltpu.roll(rows, 47, 1), 0.0))
            for c in range(2):
                grid[c, 0:25] = rows[64 * c : 64 * c + 25]
                grid[c, 25:72] = jnp.zeros((47, 128), F32)
                grid[c, 72:96] = rows[64 * c + 25 : 64 * c + BOX]
                thirds = pack(*(grid[c, pl.ds(r, 24, stride=4), :] for r in range(4)))
                for t in range(3):
                    xin[3 * c + jj, pl.ds(2 * t + j, 24, stride=6), :] = thirds[t]

    @pl.when(jnp.logical_not(active))
    def _():
        xin[...] = jnp.zeros((6, 144, 128), F32)

    pltpu.make_async_copy(xin, out_hbm, s_out.at[0]).start()

    for k in range(6):
        valid, _, target = start_of(k)

        @pl.when(both(valid, jnp.logical_not(is_me(target))))
        def _():
            await_bytes(xt.at[k], s_init.at[k])

    for n in range(2):

        @pl.when(jnp.logical_not(is_me(v_target(n))))
        def _():
            await_bytes(vp, s_v.at[n])

    scattered(cur, 0)
    scattered(hy, 1)

    @pl.when(summing)
    def _():
        await_bytes(sbuf.at[0, pl.ds(0, 255)], s_p.at[1])
        await_bytes(full.at[pl.ds(0, 67)], s_p.at[0])
        for t in range(8):

            @pl.when(p != t)
            def _():
                await_bytes(qs.at[pl.ds(96 * t, 96)], s_o.at[t])

    await_bytes(xin, s_out.at[0])

    @pl.when(summing)
    def _():
        await_bytes(efull.at[pl.ds(0, 67)], r_p.at[1])

    @pl.when(jnp.logical_not(summing))
    def _():
        await_bytes(efull, r_p.at[1])

    e = added([efull[n] for n in range(68)])
    energy_ref[...] = pltpu.roll(e, 128 - 2 * p, 1)[:, :2]
    weights = jax.nn.sigmoid((fermi_ref[0] - e) / TEMPER)
    weighted = jnp.where(lane < BANDS, weights * e, 0.0)
    band_energy_ref[...] = jnp.sum(weighted, axis=1, keepdims=True) / float(BANDS)


def call(lower, upper, fermi, height, x, v):
    smem = pl.BlockSpec(memory_space=pltpu.SMEM)
    hbm = pl.BlockSpec(memory_space=pl.ANY)
    vmem = pl.BlockSpec(memory_space=pltpu.VMEM)
    sem = pltpu.SemaphoreType.DMA
    consts = tables()

    def buf(*shape):
        return pltpu.VMEM(shape, F32)

    return pl.pallas_call(
        kernel,
        out_shape=(
            jax.ShapeDtypeStruct((6, 144, 128), F32),
            jax.ShapeDtypeStruct((1, 2), F32),
            jax.ShapeDtypeStruct((1, 1), F32),
        ),
        in_specs=[smem] * 3 + [hbm] * 9,
        out_specs=(hbm, vmem, vmem),
        scratch_shapes=[
            buf(6, 144, 128),
            buf(2, 96, 128),
            pltpu.VMEM((3, 96), jnp.int32),
            buf(3, 96, 96),
            buf(3, 72, 128),
            buf(6, 72, 128),
            buf(6, 96, 128),
            buf(128, 1024),
            *[pltpu.VMEM(t.shape, BF16) for t in consts],
            buf(6, 56, 128),
            buf(8, 56, 128),
            buf(8, 64, 128),
            buf(8, 64, 128),
            buf(8, 64, 128),
            buf(8, 64, 128),
            buf(8, 64, 128),
            buf(2, 384, 128),
            buf(2, 7, 24, 128),
            buf(2, 7, 24, 128),
            buf(2, 384, 128),
            buf(2, 768, 128),
            pltpu.VMEM((32, 6144), BF16),
            pltpu.VMEM((32, 6144), BF16),
            buf(4, 128),
            buf(68, 4, 128),
            buf(1, 128),
            buf(68, 1, 128),
            buf(768, 128),
            buf(4, 96, 128),
            sem((3,)),
            sem((1,)),
            sem((6,)),
            sem((6,)),
            sem((8,)),
            sem((4,)),
            sem((2,)),
            sem((2,)),
            sem((2,)),
            sem((2,)),
            sem((2,)),
            sem((2, 32)),
            sem((2,)),
            sem((2,)),
            sem((2,)),
            sem((8,)),
            sem((1,)),
            pltpu.SemaphoreType.REGULAR,
        ],
        compiler_params=pltpu.CompilerParams(
            has_side_effects=True, collective_id=0, vmem_limit_bytes=60 * 2**20
        ),
    )(lower, upper, fermi, height, x, v, *[jnp.asarray(t) for t in consts])


def local(start_bands, potential, half_height, lower_bound, upper_bound, fermi_level):
    x = start_bands.reshape(2, 2, 3, 72, 128).transpose(0, 2, 3, 1, 4).reshape(6, 144, 128)
    v = potential.transpose(2, 0, 1)
    out, energies, band_energy = call(lower_bound, upper_bound, fermi_level, half_height, x, v)
    out = out.reshape(2, 3, 72, 2, 128).transpose(0, 3, 1, 2, 4).reshape(2, 2, 3, NG * NG)
    return out, energies.reshape(2), band_energy.reshape(1)


def solution(mesh):
    placed = (P(None, "band", "fft", None), P(None, None, "fft"), P("fft", None), P(), P(), P())
    return jax.shard_map(
        local,
        mesh=mesh,
        in_specs=placed,
        out_specs=(P(None, "band", "fft", None), P("band"), P()),
        check_vma=False,
    )
```

```python
import math

import jax
import jax.numpy as jnp
import ml_dtypes
import numpy as np
from jax import lax
from jax.experimental import pallas as pl
from jax.experimental.pallas import tpu as pltpu
from jax.sharding import PartitionSpec as P

NG = 96
CELLS = float(NG**3)
BOX = 49
KIN = 12.0 / 24**2
TEMPER = 0.5
BANDS = 16
OFFSETS = sorted(
    ((dy, dx, dz) for dy in range(4) for dx in range(4) for dz in range(8)),
    key=lambda d: -(min(d[0], 4 - d[0]) + min(d[1], 4 - d[1]) + min(d[2], 8 - d[2])),
)
FAR_FIRST = (7, 6, 5, 3, 4, 2, 1, 0)
ACTIVE = (*range(9), *range(24, 32))
MEMBERS = 16
HOLDERS = 7
ZP = 3
F32, BF16 = jnp.float32, jnp.bfloat16
MESH = pl.DeviceIdType.MESH


def box_frequency():
    r = np.arange(BOX)
    return np.where(r <= 24, r, r - BOX)


def halves(table):
    table = table.astype(np.float32)
    high = table.astype(ml_dtypes.bfloat16)
    low = (table - high.astype(np.float32)).astype(ml_dtypes.bfloat16)
    return high, low


def tables():
    freq = box_frequency()
    angle = 2.0 * math.pi / NG * ((np.arange(NG)[:, None] * freq[None, :]) % NG)
    cosine, sine = np.cos(angle), np.sin(angle)
    ahead = np.zeros((192, 64))
    ahead[:96, :BOX], ahead[96:, :BOX] = cosine, sine
    back = np.zeros((128, 96))
    back[:BOX], back[64 : 64 + BOX] = cosine.T, sine.T
    lanes = np.zeros((128, 256))
    lanes[:BOX, :96], lanes[:BOX, 128:224] = cosine.T, sine.T
    lanes[64 : 64 + BOX, :96], lanes[64 : 64 + BOX, 128:224] = -sine.T, cosine.T
    lanes_back = lanes.T.copy()
    plane = np.arange(NG).reshape(MEMBERS, 2, ZP)

    def left(t):
        high, low = halves(t)
        return np.concatenate([high, high, low], axis=1)

    def right(t):
        high, low = halves(t)
        return np.concatenate([high, high, low], axis=0)

    z_ahead = [np.concatenate([ahead[plane[:, h].ravel()], ahead[96 + plane[:, h].ravel()]]) for h in range(2)]
    z_back = [back[:, plane[:, h].ravel()] for h in range(2)]
    return (
        np.stack([left(t) for t in z_ahead]),
        left(ahead),
        np.stack([left(t) for t in z_back]),
        left(back),
        right(lanes),
        right(lanes_back),
    )


def split(x):
    high = x.astype(BF16)
    return high, (x - high.astype(F32)).astype(BF16)


def pieces(x, axis):
    high, low = split(x)
    return jnp.concatenate([high, low, high], axis=axis)


def dot(a, b):
    return jnp.dot(a, b, preferred_element_type=F32)


def dot_t(a, b):
    return lax.dot_general(a, b, (((1,), (1,)), ((), ())), preferred_element_type=F32)


def kernel(
    lower_ref,
    upper_ref,
    fermi_ref,
    height_hbm,
    x_hbm,
    v_hbm,
    tz_hbm,
    tx_hbm,
    tzb_hbm,
    txb_hbm,
    ty_hbm,
    tyb_hbm,
    out_hbm,
    energy_ref,
    band_energy_ref,
    xin,
    grid,
    height_ref,
    vin,
    vp,
    vb,
    vfull,
    acc,
    tz,
    tx,
    tzb,
    txb,
    ty,
    tyb,
    xt,
    x0,
    cur,
    prev,
    hy,
    inside,
    kin,
    sbuf,
    rbuf,
    bbuf,
    kbuf,
    gy,
    bh,
    bl,
    part,
    full,
    epart,
    efull,
    qs,
    ob,
    s_in,
    s_out,
    s_t,
    s_init,
    r_init,
    s_v,
    r_v,
    s_f,
    r_f,
    s_b,
    r_b,
    s_g,
    r_g,
    s_p,
    r_p,
    s_o,
    r_o,
    planes_in,
):
    p = lax.axis_index("band")
    i = lax.axis_index("fft")

    def quot(a, n):
        return a // n if isinstance(a, int) else lax.div(a, jnp.int32(n))

    def mod(a, n):
        return a % n if isinstance(a, int) else lax.rem(a, jnp.int32(n))

    def both(a, b):
        return jnp.logical_and(a, b)

    y, core = quot(p, 2), mod(p, 2)
    y2, yl = quot(y, 2), mod(y, 2)
    gx, gzz = quot(i, 8), mod(i, 8)
    x2, xl = quot(gx, 2), mod(gx, 2)
    gz, zl = quot(gzz, 2), mod(gzz, 2)
    band = 8 * y2 + 4 * x2 + gz
    xr = 2 * yl + mod(xl + yl, 2)
    zr = 2 * core + mod(zl + core, 2)
    place = 4 * xr + zr
    me = 4 * mod(xr + 2 * x2, 4) + mod(zr + 2 * quot(gz, 2), 4)
    chip = 2 * xr + zr - 2
    is_k = both(core == 1, chip < HOLDERS)
    active = jnp.logical_or(i <= 8, i >= 24)
    lone = i == 8

    def dev(pp, ii):
        return {"band": pp, "fft": ii}

    def at_place(yy, xx, zz, xr_, zr_):
        c = quot(zr_, 2)
        return dev(
            4 * yy + 2 * quot(xr_, 2) + c,
            16 * xx + 8 * mod(quot(xr_ + 1, 2), 2) + 2 * zz + mod(quot(zr_ + 1, 2), 2),
        )

    def holder(b, s):
        return at_place(quot(b, 8), mod(quot(b, 4), 2), mod(b, 4), quot(s, 2), 2 + mod(s, 2))

    def mine_at(n):
        return at_place(y2, x2, gz, n // 4, n % 4)

    def across(d, c):
        yy, xx, zz = mod(yl + d // 4, 2), mod(xl + d // 2 % 2, 2), mod(zl + d % 2, 2)
        return (
            2 * yy + mod(xx + yy, 2),
            2 * c + mod(zz + c, 2),
            dev(4 * y2 + 2 * yy + c, 16 * x2 + 8 * xx + 2 * gz + zz),
        )

    def is_me(where):
        return both(where["band"] == p, where["fft"] == i)

    def remote(src, dst, ss, rs, where):
        return pltpu.make_async_remote_copy(
            src_ref=src, dst_ref=dst, send_sem=ss, recv_sem=rs, device_id=where, device_id_type=MESH
        )

    def await_bytes(ref, sem):
        pltpu.make_async_copy(ref, ref, sem).wait()

    for src, dst, n in ((x_hbm, xin, 0), (v_hbm, vin, 1), (height_hbm, height_ref, 2)):
        pltpu.make_async_copy(src, dst, s_in.at[n]).start()
    for n, (src, dst) in enumerate(
        ((tz_hbm, tz), (tx_hbm, tx), (tzb_hbm, tzb), (txb_hbm, txb), (ty_hbm, ty), (tyb_hbm, tyb))
    ):
        pltpu.make_async_copy(src, dst, s_t.at[n]).start()

    barrier = pltpu.get_barrier_semaphore()

    def tell(where):
        pl.semaphore_signal(barrier, inc=1, device_id=where, device_id_type=MESH)

    def kx_of_slot(a):
        q = 8 * chip + a
        return q < BOX, jnp.where(q <= 24, q, q + 47)

    @pl.when(is_k)
    def _():
        for a in range(8):
            held, kx = kx_of_slot(a)
            native = dev(quot(band, 2), quot(kx, 3))

            @pl.when(both(held, jnp.logical_not(is_me(native))))
            def _():
                tell(native)

    for h in range(2):
        source = dev(2 * y + quot(gz, 2), 2 * me + h)

        @pl.when(jnp.logical_not(is_me(source)))
        def _():
            tell(source)

    for n in range(MEMBERS):

        @pl.when(place != n)
        def _():
            tell(mine_at(n))

    def counterpart(n):
        return at_place(
            mod(y2 + n // 8, 2), mod(x2 + (n // 4) % 2, 2), mod(gz + n % 4, 4), xr, zr
        )

    for n in range(1, 16):
        tell(counterpart(n))

    def start_of(k):
        j, jj = k // 3, k % 3
        kx = 3 * i + jj
        valid = jnp.logical_or(kx <= 24, kx >= 72)
        q = jnp.where(kx <= 24, kx, kx - 47)
        s = jnp.minimum(jnp.maximum(quot(q, 8), 0), HOLDERS - 1)
        return valid, mod(q, 8), holder(2 * p + j, s)

    def v_target(n):
        xx = mod(quot(gx, 2) + yl, 2)
        return at_place(y2, xx, 2 * core + n, mod(gx + 2 * xx, 4), mod(quot(gzz, 2) + 2 * core, 4))

    expected = jnp.int32(30)
    for k in range(6):
        valid, _, target = start_of(k)
        expected = expected + both(valid, jnp.logical_not(is_me(target))).astype(jnp.int32)
    for n in range(2):
        expected = expected + jnp.logical_not(is_me(v_target(n))).astype(jnp.int32)

    lane = lax.broadcasted_iota(jnp.int32, (1, 128), 1)
    sign = jnp.where(lane < 64, -1.0, 1.0).astype(F32)

    def swap(x):
        return pltpu.roll(x, 64, 1)

    def boxed_lanes(x):
        return jnp.where(lane < 25, x, jnp.where(lane < BOX, pltpu.roll(x, 128 - 47, 1), 0.0))

    def unpack(t0, t1, t2):
        return (
            t0,
            jnp.where(lane < 32, pltpu.roll(t0, 32, 1), pltpu.roll(t1, 32, 1)),
            jnp.where(lane < 64, pltpu.roll(t1, 64, 1), pltpu.roll(t2, 64, 1)),
            pltpu.roll(t2, 96, 1),
        )

    def pack(o0, o1, o2, o3):
        return (
            jnp.where(lane < 96, o0, pltpu.roll(o1, 96, 1)),
            jnp.where(lane < 64, pltpu.roll(o1, 96, 1), pltpu.roll(o2, 64, 1)),
            jnp.where(lane < 32, pltpu.roll(o2, 64, 1), pltpu.roll(o3, 32, 1)),
        )

    await_bytes(xin, s_in.at[0])
    await_bytes(height_ref, s_in.at[2])
    for k in range(6):
        j, jj = k // 3, k % 3
        for c in range(2):
            quarter = unpack(*(xin[3 * c + jj, pl.ds(2 * t + j, 24, stride=6), :] for t in range(3)))
            for r in range(4):
                grid[c, pl.ds(r, 24, stride=4), :] = boxed_lanes(quarter[r])
        pad = jnp.zeros((15, 128), F32)
        rows = jnp.concatenate([grid[0, 0:25], grid[0, 72:96], pad, grid[1, 0:25], grid[1, 72:96], pad], axis=0)
        xt[k] = rows.T[:56]
    for jj in range(3):
        h = height_ref[jj : jj + 1, :].astype(F32)
        h = boxed_lanes(jnp.concatenate([h, jnp.zeros((1, 32), F32)], axis=1))
        h = jnp.where(lane < BOX, h, -1.0)
        h = jnp.where(lane < 64, h, pltpu.roll(h, 64, 1))
        for j in range(2):
            xt[3 * j + jj, BOX : BOX + 1, :] = h
    await_bytes(vin, s_in.at[1])
    for z in range(3):
        grid[0] = jnp.concatenate([vin[z], jnp.zeros((96, 32), F32)], axis=1)
        thirds = pack(*(grid[0, pl.ds(r, 24, stride=4), :] for r in range(4)))
        for t in range(3):
            vp[z, 24 * t : 24 * t + 24, :] = thirds[t]

    pl.semaphore_wait(barrier, expected)

    for k in range(6):
        valid, slot, target = start_of(k)

        @pl.when(both(valid, is_me(target)))
        def _():
            pltpu.make_async_copy(xt.at[k], x0.at[slot], r_init.at[slot]).start()

        @pl.when(both(valid, jnp.logical_not(is_me(target))))
        def _():
            remote(xt.at[k], x0.at[slot], s_init.at[k], r_init.at[slot], target).start()

    for n in range(2):
        target = v_target(n)
        home = vb.at[pl.ds(3 * mod(i, 2), 3)]

        @pl.when(is_me(target))
        def _():
            pltpu.make_async_copy(vp, home, r_v.at[mod(i, 2)]).start()

        @pl.when(jnp.logical_not(is_me(target)))
        def _():
            remote(vp, home, s_v.at[n], r_v.at[mod(i, 2)], target).start()

    for n in range(1, 16):
        pl.semaphore_signal(planes_in, inc=1, device_id=counterpart(n), device_id_type=MESH)

    for n, dst in enumerate((tz, tx, tzb, txb, ty, tyb)):
        await_bytes(dst, s_t.at[n])

    @pl.when(is_k)
    def _():
        row = lax.broadcasted_iota(jnp.int32, (64, 128), 0)
        col_ = lax.broadcasted_iota(jnp.int32, (64, 128), 1) % 64
        fz = jnp.where(row <= 24, row, row - BOX)
        fy = jnp.where(col_ <= 24, col_, col_ - BOX)
        in_box = jnp.logical_and(row < BOX, col_ < BOX)
        yz = (fz * fz + fy * fy).astype(F32)
        absz = jnp.abs(fz).astype(F32)

        def plane(a, _):
            q = 8 * chip + a

            @pl.when(q < BOX)
            def _():
                await_bytes(x0.at[a], r_init.at[a])
                fx = jnp.where(q <= 24, q, q - BOX)
                data = x0[a]
                data = jnp.concatenate([data, jnp.zeros((8, 128), F32)], axis=0)
                keep = both(in_box, absz <= data[BOX : BOX + 1])
                cur[a] = jnp.where(keep, data, 0.0)
                inside[a] = jnp.where(keep, 1.0 / CELLS, 0.0)
                kin[a] = jnp.where(keep, KIN * (yz + (fx * fx).astype(F32)), 0.0)

            @pl.when(q >= BOX)
            def _():
                zero = jnp.zeros((64, 128), F32)
                cur[a] = zero
                inside[a] = zero
                kin[a] = zero

            prev[a] = jnp.zeros((64, 128), F32)
            return 0

        lax.fori_loop(0, 8, plane, 0)

    def message(m):
        return pl.ds(pl.multiple_of(24 * m, 8), 24)

    def forward():
        @pl.when(is_k)
        def _():
            x = pieces(jnp.concatenate([cur[a] for a in range(8)], axis=1), 0)
            for h in range(2):
                out = dot(tz[h], x)
                for a in range(8):
                    c, s = out[:48, 128 * a : 128 * a + 128], out[48:, 128 * a : 128 * a + 128]
                    sbuf[h, pl.ds(a, 48, stride=8), :] = c + sign * swap(s)

                home = rbuf.at[h, chip]
                for d in FAR_FIRST:
                    for c in range(2):
                        xr_, zr_, target = across(d, c)
                        slab = 4 * mod(xr_ + 2 * x2, 4) + mod(zr_ + 2 * quot(gz, 2), 4)
                        src = sbuf.at[h, message(slab)]
                        if d == 0 and c == 1:
                            pltpu.make_async_copy(src, home, r_f.at[h]).start()
                        else:
                            remote(src, home, s_f.at[h], r_f.at[h], target).start()

    def middle(first):
        zero8 = jnp.zeros((8, 128), F32)
        for h in range(2):
            await_bytes(rbuf.at[h], r_f.at[h])
            d = jnp.concatenate(
                [
                    jnp.concatenate(
                        [rbuf[h, s, 8 * z : 8 * z + 8, :] for s in range(HOLDERS)] + [zero8], axis=0
                    )
                    for z in range(ZP)
                ],
                axis=1,
            )
            out = dot(tx[...], pieces(d, 0))
            rows = jnp.concatenate(
                [
                    out[:96, 128 * z : 128 * z + 128] + sign * swap(out[96:, 128 * z : 128 * z + 128])
                    for z in range(ZP)
                ],
                axis=0,
            )
            psi = dot(pieces(rows, 1), ty[...])

            @pl.when(first)
            def _():
                await_bytes(vb.at[pl.ds(3 * h, 3)], r_v.at[h])
                for z in range(3 * h, 3 * h + 3):
                    quarter = unpack(*(vb[z, 24 * t : 24 * t + 24, :] for t in range(3)))
                    for r in range(4):
                        vfull[z, pl.ds(r, 24, stride=4), :] = jnp.where(lane < NG, quarter[r], 0.0)

            v = jnp.concatenate([vfull[3 * h + z] for z in range(ZP)], axis=0)
            psi = psi * jnp.concatenate([v, v], axis=1)
            rows = dot(pieces(psi, 1), tyb[...])
            d = jnp.concatenate([rows[96 * z : 96 * z + 96] for z in range(ZP)], axis=1)
            out = dot(txb[...], pieces(d, 0))
            for z in range(ZP):
                o = out[:64, 128 * z : 128 * z + 128] - sign * swap(out[64:, 128 * z : 128 * z + 128])
                for s in range(HOLDERS):
                    bbuf[h, s, 8 * z : 8 * z + 8, :] = o[8 * s : 8 * s + 8]

            home = kbuf.at[h, message(me)]
            for d in FAR_FIRST:
                xr_, zr_, target = across(d, 1)
                s = 2 * xr_ + zr_ - 2
                src = bbuf.at[h, jnp.minimum(s, HOLDERS - 1)]
                held = s < HOLDERS
                if d == 0:

                    @pl.when(is_k)
                    def _():
                        pltpu.make_async_copy(src, home, r_b.at[h]).start()

                    held = both(held, core == 0)

                @pl.when(held)
                def _():
                    remote(src, home, s_b.at[h], r_b.at[h], target).start()

    def backward(finish):
        @pl.when(is_k)
        def _():
            for h in range(2):
                await_bytes(kbuf.at[h], r_b.at[h])
                d = jnp.concatenate([kbuf[h, pl.ds(a, 48, stride=8), :] for a in range(8)], axis=1)
                term = dot(tzb[h], pieces(d, 0))
                acc[...] = acc[...] + term if h else term
            for a in range(8):
                f = acc[:64, 128 * a : 128 * a + 128] - sign * swap(acc[64:, 128 * a : 128 * a + 128])
                finish(a, kin[a] * cur[a] + inside[a] * f)
            for h in range(2):
                await_bytes(sbuf.at[h, pl.ds(0, 24 * (MEMBERS - 1))], s_f.at[h])
                await_bytes(bbuf.at[h, pl.ds(0, HOLDERS - 1)], s_b.at[h])

        @pl.when(jnp.logical_not(is_k))
        def _():
            for h in range(2):
                await_bytes(bbuf.at[h], s_b.at[h])

    center = 0.5 * (upper_ref[0] + lower_ref[0])
    half_width = 0.5 * (upper_ref[0] - lower_ref[0])

    def step(k, _):
        forward()
        middle(k == 0)
        alpha = jnp.where(k == 0, 1.0, 2.0).astype(F32)
        beta = jnp.where(k == 0, 0.0, 1.0).astype(F32)

        def finish(a, h):
            old = cur[a]
            new = alpha * (h - center * old) / half_width - beta * prev[a]
            prev[a] = old
            cur[a] = new

        backward(finish)
        return 0

    lax.fori_loop(0, 3, step, 0)

    on_zero = core == 0
    summing = both(on_zero, active)

    def for_rows(do):
        @pl.when(is_k)
        def _():
            for a in range(8):
                held, kx = kx_of_slot(a)
                home, jj = quot(kx, 3), mod(kx, 3)

                @pl.when(held)
                def _():
                    for n in range(4):
                        do(a, n, jj, dev(2 * n, home))

    def scatter(src, w):
        def one(a, n, jj, target):
            dst = gy.at[w, pl.ds(pl.multiple_of(256 * jj + 16 * band, 8), 16)]
            remote(src.at[a, pl.ds(16 * n, 16)], dst, s_g.at[w, 4 * a + n], r_g.at[w], target).start()

        for_rows(one)

    def scattered(src, w):
        def one(a, n, jj, target):
            await_bytes(src.at[a, pl.ds(16 * n, 16)], s_g.at[w, 4 * a + n])

        for_rows(one)

    def all_rows(w):
        @pl.when(lone)
        def _():
            await_bytes(gy.at[w, pl.ds(0, 256)], r_g.at[w])

        @pl.when(jnp.logical_not(lone))
        def _():
            await_bytes(gy.at[w], r_g.at[w])

        rows = []
        for jj in range(3):
            for r in range(16):
                x = gy[w, pl.ds(256 * jj + r, BANDS, stride=16), :]
                rows.append(jnp.where(lone, 0.0, x) if jj else x)
        a = jnp.concatenate(rows, axis=1)
        b = jnp.concatenate([-sign * swap(x) for x in rows], axis=1)
        return jnp.concatenate([a, b], axis=0)

    my_slot = jnp.minimum(jnp.where(i <= 8, i, jnp.maximum(i - 15, 0)), 16)

    def added(terms):
        while len(terms) > 1:
            terms = [a + b for a, b in zip(terms[::2], terms[1::2])] + ([terms[-1]] if len(terms) % 2 else [])
        return terms[0]

    lane2 = lax.broadcasted_iota(jnp.int32, (16, 128), 1)

    def inverse_rows(g):
        row = lax.broadcasted_iota(jnp.int32, (32, 128), 0)
        ln = lax.broadcasted_iota(jnp.int32, (32, 128), 1)
        top = jnp.where(lane2 < 16, g, -g)
        bottom = jnp.where(lane2 < 16, pltpu.roll(g, 112, 1), pltpu.roll(g, 16, 1))
        m = jnp.where(ln < 32, jnp.concatenate([top, bottom], 0), 0.0)
        m = m + jnp.where(ln == row + 32, 1.0, 0.0)
        for j in range(32):
            pivot = m[j : j + 1, :]
            factor = m[:, j : j + 1] * (1.0 / pivot[:, j : j + 1])
            m = m - jnp.where(row > j, factor, 0.0) * pivot
        diag = jnp.sum(jnp.where(ln == row, m, 0.0), axis=1, keepdims=True)
        u = m[:16] / jnp.sqrt(diag[:16])
        return jnp.where(lane2 < 32, pltpu.roll(u, 96, 1), 0.0)

    pl.semaphore_wait(planes_in, 15)
    scatter(cur, 0)
    forward()
    middle(False)

    def keep(a, h):
        hy[a] = h

    backward(keep)
    scatter(hy, 1)

    @pl.when(summing)
    def _():
        high, low = split(all_rows(0))
        bh[...] = high
        bl[...] = low
        g = (dot_t(bh[:BANDS], high) + dot_t(bh[:BANDS], low) + dot_t(bl[:BANDS], high)) * (1.0 / CELLS)
        g = jnp.concatenate([g, jnp.zeros((BANDS, 96), F32)], axis=1)
        packed = g[0:4]
        for n in range(1, 4):
            packed = packed + pltpu.roll(g[4 * n : 4 * n + 4], 32 * n, 1)
        part[...] = packed
        full[17 * y + my_slot] = packed
        for dy in (2, 1, 3, 0):
            pp = 2 * mod(y + dy, 4)
            for ii in ACTIVE:

                def send():
                    remote(part, full.at[17 * y + my_slot], s_p.at[0], r_p.at[0], dev(pp, ii)).start()

                if dy:
                    send()
                else:
                    pl.when(i != ii)(send)

        await_bytes(full.at[pl.ds(0, 67)], r_p.at[0])
        total = added([full[n] for n in range(68)])

        g = jnp.concatenate([total] + [pltpu.roll(total, 128 - 32 * n, 1) for n in range(1, 4)], axis=0)
        u_rows = inverse_rows(jnp.where(lane2 < 32, g, 0.0))
        w_high, w_low = split(jnp.where(lane2 < 16, u_rows, -u_rows)[:, :32])

        def rotated(high, low):
            return dot(w_high, high) + dot(w_high, low) + dot(w_low, high)

        q = rotated(bh[...], bl[...])
        for n in range(48):
            qs[pl.ds(n, BANDS, stride=48), :] = q[:, 128 * n : 128 * n + 128]
        hq = rotated(*split(all_rows(1)))
        e = q[:, :128] * hq[:, :128]
        for n in range(1, 48):
            e = e + q[:, 128 * n : 128 * n + 128] * hq[:, 128 * n : 128 * n + 128]
        e = jnp.sum(e, axis=1, keepdims=True) * (1.0 / CELLS)
        row = lax.broadcasted_iota(jnp.int32, (16, 128), 0)
        epart[...] = jnp.sum(jnp.where(lane2 == row, e, 0.0), axis=0, keepdims=True)
        mine = 17 * y + my_slot
        efull[mine] = epart[...]
        for dy, dx, dz in OFFSETS:
            pp, ii = 2 * mod(y + dy, 4), 8 * mod(gx + dx, 4) + mod(gzz + dz, 8)
            for c in range(1 if dy + dx + dz == 0 else 0, 2):
                remote(epart, efull.at[mine], s_p.at[1], r_p.at[1], dev(pp + c, ii)).start()

        for t in range(8):
            src = qs.at[pl.ds(96 * t, 96)]

            @pl.when(p == t)
            def _():
                pltpu.make_async_copy(src, ob.at[y], r_o.at[0]).start()

            @pl.when(p != t)
            def _():
                remote(src, ob.at[y], s_o.at[t], r_o.at[0], dev(t, i)).start()

    @pl.when(active)
    def _():
        await_bytes(ob, r_o.at[0])
        zero = jnp.zeros((64, 128), F32)
        low_lanes, high_lanes = lane < 25, jnp.logical_and(lane >= 72, lane < 96)
        for k in range(6):
            j, jj = k // 3, k % 3
            rows = jnp.concatenate([ob[n, 16 * k : 16 * k + 16, :] for n in range(4)] + [zero], axis=0)
            if jj:
                rows = jnp.where(lone, 0.0, rows)
            rows = rows.T
            rows = jnp.where(low_lanes, rows, jnp.where(high_lanes, pltpu.roll(rows, 47, 1), 0.0))
            for c in range(2):
                grid[c, 0:25] = rows[64 * c : 64 * c + 25]
                grid[c, 25:72] = jnp.zeros((47, 128), F32)
                grid[c, 72:96] = rows[64 * c + 25 : 64 * c + BOX]
                thirds = pack(*(grid[c, pl.ds(r, 24, stride=4), :] for r in range(4)))
                for t in range(3):
                    xin[3 * c + jj, pl.ds(2 * t + j, 24, stride=6), :] = thirds[t]

    @pl.when(jnp.logical_not(active))
    def _():
        xin[...] = jnp.zeros((6, 144, 128), F32)

    pltpu.make_async_copy(xin, out_hbm, s_out.at[0]).start()

    for k in range(6):
        valid, _, target = start_of(k)

        @pl.when(both(valid, jnp.logical_not(is_me(target))))
        def _():
            await_bytes(xt.at[k], s_init.at[k])

    for n in range(2):

        @pl.when(jnp.logical_not(is_me(v_target(n))))
        def _():
            await_bytes(vp, s_v.at[n])

    scattered(cur, 0)
    scattered(hy, 1)

    @pl.when(summing)
    def _():
        await_bytes(sbuf.at[0, pl.ds(0, 255)], s_p.at[1])
        await_bytes(full.at[pl.ds(0, 67)], s_p.at[0])
        for t in range(8):

            @pl.when(p != t)
            def _():
                await_bytes(qs.at[pl.ds(96 * t, 96)], s_o.at[t])

    await_bytes(xin, s_out.at[0])

    @pl.when(summing)
    def _():
        await_bytes(efull.at[pl.ds(0, 67)], r_p.at[1])

    @pl.when(jnp.logical_not(summing))
    def _():
        await_bytes(efull, r_p.at[1])

    e = added([efull[n] for n in range(68)])
    energy_ref[...] = pltpu.roll(e, 128 - 2 * p, 1)[:, :2]
    weights = jax.nn.sigmoid((fermi_ref[0] - e) / TEMPER)
    weighted = jnp.where(lane < BANDS, weights * e, 0.0)
    band_energy_ref[...] = jnp.sum(weighted, axis=1, keepdims=True) / float(BANDS)


def call(lower, upper, fermi, height, x, v):
    smem = pl.BlockSpec(memory_space=pltpu.SMEM)
    hbm = pl.BlockSpec(memory_space=pl.ANY)
    vmem = pl.BlockSpec(memory_space=pltpu.VMEM)
    sem = pltpu.SemaphoreType.DMA
    consts = tables()

    def buf(*shape):
        return pltpu.VMEM(shape, F32)

    return pl.pallas_call(
        kernel,
        out_shape=(
            jax.ShapeDtypeStruct((6, 144, 128), F32),
            jax.ShapeDtypeStruct((1, 2), F32),
            jax.ShapeDtypeStruct((1, 1), F32),
        ),
        in_specs=[smem] * 3 + [hbm] * 9,
        out_specs=(hbm, vmem, vmem),
        scratch_shapes=[
            buf(6, 144, 128),
            buf(2, 96, 128),
            pltpu.VMEM((3, 96), jnp.int32),
            buf(3, 96, 96),
            buf(3, 72, 128),
            buf(6, 72, 128),
            buf(6, 96, 128),
            buf(128, 1024),
            *[pltpu.VMEM(t.shape, BF16) for t in consts],
            buf(6, 56, 128),
            buf(8, 56, 128),
            buf(8, 64, 128),
            buf(8, 64, 128),
            buf(8, 64, 128),
            buf(8, 64, 128),
            buf(8, 64, 128),
            buf(2, 384, 128),
            buf(2, 7, 24, 128),
            buf(2, 7, 24, 128),
            buf(2, 384, 128),
            buf(2, 768, 128),
            pltpu.VMEM((32, 6144), BF16),
            pltpu.VMEM((32, 6144), BF16),
            buf(4, 128),
            buf(68, 4, 128),
            buf(1, 128),
            buf(68, 1, 128),
            buf(768, 128),
            buf(4, 96, 128),
            sem((3,)),
            sem((1,)),
            sem((6,)),
            sem((6,)),
            sem((8,)),
            sem((4,)),
            sem((2,)),
            sem((2,)),
            sem((2,)),
            sem((2,)),
            sem((2,)),
            sem((2, 32)),
            sem((2,)),
            sem((2,)),
            sem((2,)),
            sem((8,)),
            sem((1,)),
            pltpu.SemaphoreType.REGULAR,
        ],
        compiler_params=pltpu.CompilerParams(
            has_side_effects=True, collective_id=0, vmem_limit_bytes=60 * 2**20
        ),
    )(lower, upper, fermi, height, x, v, *[jnp.asarray(t) for t in consts])


def local(start_bands, potential, half_height, lower_bound, upper_bound, fermi_level):
    x = start_bands.reshape(2, 2, 3, 72, 128).transpose(0, 2, 3, 1, 4).reshape(6, 144, 128)
    v = potential.transpose(2, 0, 1)
    out, energies, band_energy = call(lower_bound, upper_bound, fermi_level, half_height, x, v)
    out = out.reshape(2, 3, 72, 2, 128).transpose(0, 3, 1, 2, 4).reshape(2, 2, 3, NG * NG)
    return out, energies.reshape(2), band_energy.reshape(1)


def solution(mesh):
    placed = (P(None, "band", "fft", None), P(None, None, "fft"), P("fft", None), P(), P(), P())
    return jax.shard_map(
        local,
        mesh=mesh,
        in_specs=placed,
        out_specs=(P(None, "band", "fft", None), P("band"), P()),
        check_vma=False,
    )
```
